32 devices in a mesh: ao: 8 (over y, x, core), aux: 4 (over z).
Axes of the slice: x: 2, y: 2, z: 4, core: 2. Of those that a mesh axis runs over, the one named last changes fastest.
Arguments:
- blocks: bfloat16 [48, 256, 128, 128], P('ao', 'aux'), may hold values from -6 to 6
- pairs: int32 [48, 2], P('ao'), may hold values from 0 to 79, as said below
- counts: int32 [8], P('ao'), may hold values from 1 to 6, as said below
- owned_blocks: int32 [80], P('ao'), may hold values from 0 to 79, as said below
- occ_coef: bfloat16 [80, 8, 128], P('ao'), may hold values from -0.5 to 0.5
- vir_coef: bfloat16 [10240, 9216], P('ao', 'aux'), may hold values from -0.109375 to 0.109375
Outputs:
- b_tensor: bfloat16 [256, 8, 9216], P('ao', None, 'aux')
The draws below stay inside these ranges and needn't reach their ends.
Inputs may be any that keep to these rules, and one draw needn't show every extreme that they name: `pairs`: among the used slots of one ao index, at most 3 have nu blocks whose rows one owner holds; in every draw some index reaches 3. `counts`: some ao index uses all 6 slots in every draw. `owned_blocks`: every atom block appears exactly once.
All inputs are finite; a program needn't handle non-finite values.
Results may differ from the reference program's by a relative error of at most 0.014.
Values may be sent and summed in bfloat16 or wider, within the bound.
A program may use at most 128 MiB of HBM per device.

```python
import jax
import jax.numpy as jnp
from jax import lax

BLK = 128
BLK_DEV = 10
OCC = 8
SLOTS = 6
NBLK = 80
NAO = 10240
PS = 256
V = 9216
CAP = 3
ALL_SLOTS = 48
N_AO = 8


def slot_layout(key):
    perm_blocks = jax.random.permutation(jax.random.fold_in(key, 11), NBLK).astype(jnp.int32)
    used_counts = jax.random.randint(jax.random.fold_in(key, 12), (N_AO,), 1, SLOTS + 1).astype(jnp.int32)
    full_index = jax.random.randint(jax.random.fold_in(key, 13), (), 0, N_AO)
    used_counts = jnp.where(jnp.arange(N_AO) == full_index, SLOTS, used_counts).astype(jnp.int32)
    first_owner = jax.random.randint(jax.random.fold_in(key, 14), (N_AO,), 0, N_AO)
    second_owner = (first_owner + 1 + jax.random.randint(jax.random.fold_in(key, 15), (N_AO,), 0, N_AO - 1)) % N_AO
    slot_half = jnp.arange(SLOTS) // CAP
    owner_pick = jnp.where(slot_half[None, :] == 0, first_owner[:, None], second_owner[:, None])
    local_pick = jax.random.randint(jax.random.fold_in(key, 16), (N_AO, SLOTS), 0, BLK_DEV)
    second_block = perm_blocks[owner_pick * BLK_DEV + local_pick]
    first_block = jax.random.randint(jax.random.fold_in(key, 17), (N_AO, SLOTS), 0, NBLK)
    pair_list = jnp.stack([first_block, second_block], axis=-1).reshape(N_AO * SLOTS, 2).astype(jnp.int32)
    return (pair_list, used_counts, perm_blocks)


def draw_pairs(key, part):
    return slot_layout(key)[0]


def draw_counts(key, part):
    return slot_layout(key)[1]


def draw_owned_blocks(key, part):
    return slot_layout(key)[2]


def steps_of(stream_key, extent, shards, low, top_value):
    factor_of, own = 1.0, jax.random.fold_in(stream_key, 6)
    for axis_at, shards_of in shards:
        draws = jnp.exp(jax.random.uniform(jax.random.fold_in(own, axis_at), (shards_of,), jnp.float32, low / len(shards), top_value / len(shards)))
        factor_of = factor_of * jnp.repeat(draws, extent[axis_at] // shards_of).reshape([-1 if axis == axis_at else 1 for axis in range(len(extent))])
    return factor_of


def scatter_about(rng, shape, width, bound, pieces=(), kind=jnp.bfloat16):
    array = jax.random.normal(rng, shape, jnp.float32) * width
    if len(pieces) > 0:
        array = steps_of(rng, shape, pieces, -0.22, 0.18) * array
    return jnp.clip(array, min=-bound, max=bound).astype(kind)


def setup_inputs(seed: int = 0) -> dict:
    streams_of = jax.random.split(jax.random.key(seed), 7)
    blocks = scatter_about(streams_of[0], (ALL_SLOTS, PS, BLK, BLK), 1.0, 6.0, ((0, 8), (1, 4)))
    pairs = draw_pairs(jax.random.fold_in(streams_of[6], 71), 0)
    counts = draw_counts(jax.random.fold_in(streams_of[6], 71), 0)
    owned_blocks = draw_owned_blocks(jax.random.fold_in(streams_of[6], 71), 0)
    occ_coef = scatter_about(streams_of[4], (NBLK, OCC, BLK), BLK ** -0.5, 0.5, ((0, 8),))
    vir_coef = scatter_about(streams_of[5], (NAO, V), (BLK * ALL_SLOTS // 2) ** -0.5, 0.109375, ((0, 8), (1, 4)))
    return {"blocks": blocks, "pairs": pairs, "counts": counts, "owned_blocks": owned_blocks, "occ_coef": occ_coef, "vir_coef": vir_coef}


def half_slab(args):
    block, coef, in_use = args
    value = jnp.einsum("im,pmn->pin", coef.astype(jnp.float32), block.astype(jnp.float32))
    return jnp.where(in_use, value, jnp.zeros_like(value)).astype(jnp.bfloat16)


def reference(blocks, pairs, counts, owned_blocks, occ_coef, vir_coef):
    total_blocks = owned_blocks.shape[0]
    slot_total = pairs.shape[0]
    slot_count = slot_total // N_AO
    block_width = blocks.shape[2]
    positions = jnp.arange(total_blocks, dtype=jnp.int32)
    place = jnp.zeros((total_blocks,), jnp.int32).at[owned_blocks].set(positions)
    in_use = (jnp.arange(slot_count, dtype=jnp.int32)[None, :] < counts[:, None]).reshape(-1)
    row_first = place[pairs[:, 0]]
    row_second = place[pairs[:, 1]]
    slabs = lax.map(half_slab, (blocks, occ_coef[row_first], in_use))
    gathered = jax.ops.segment_sum(slabs.astype(jnp.float32), row_second, num_segments=total_blocks)
    gathered = gathered.astype(jnp.bfloat16)
    per_owner = total_blocks // N_AO
    occupied = occ_coef.shape[1]
    total = jnp.zeros((PS * occupied, vir_coef.shape[1]), jnp.float32)
    for owner_idx in range(N_AO):
        part = gathered[owner_idx * per_owner:(owner_idx + 1) * per_owner]
        left = jnp.transpose(part, (1, 2, 0, 3)).reshape(PS * occupied, per_owner * block_width)
        right = vir_coef[owner_idx * per_owner * block_width:(owner_idx + 1) * per_owner * block_width]
        term = jnp.dot(left, right, preferred_element_type=jnp.float32).astype(jnp.bfloat16)
        total = total + term.astype(jnp.float32)
    return total.reshape(PS, occupied, vir_coef.shape[1]).astype(jnp.bfloat16)
```

```python
import functools

import jax
import jax.numpy as jnp
from jax import lax
from jax.experimental import pallas as pl
from jax.experimental.pallas import tpu as pltpu
from jax.sharding import PartitionSpec as P

MESH = pl.DeviceIdType.MESH
CAP = 3
CHUNKS = 4
TAB_ROWS = 32
f32 = jnp.float32
bf16 = jnp.bfloat16


def block_place(block_ids, owned_all):
    hits = block_ids[..., None] == owned_all
    positions = jnp.arange(owned_all.shape[0], dtype=jnp.int32)
    return jnp.sum(jnp.where(hits, positions, 0), axis=-1)


def iota2(shape, axis):
    return lax.broadcasted_iota(jnp.int32, shape, axis)


def make_tables(n, slots, per_owner, chip, variants, flat, tab_ref):
    total, owned, cap = n * slots, n * per_owner, 2 * slots
    chips, most, zero_slab = n // 2, n * CAP, n * slots
    flat = flat.astype(f32)
    nu_row, live_row, own_row = flat[1:2], flat[2:3] > 0, flat[3:4]
    o0, o1 = iota2((owned, 128), 0), iota2((owned, 128), 1)
    own_col = jnp.sum(jnp.where(o0 == o1, own_row, 0.0), axis=1, keepdims=True)
    place_mu, place = (
        jnp.sum(jnp.where(own_col == row, o0.astype(f32), 0.0), axis=0, keepdims=True) for row in (flat[0:1], nu_row)
    )
    t0, t1 = iota2((total, 128), 0), iota2((total, 128), 1)
    lane = t1.astype(f32)
    lane1 = lane[0:1]
    before = t0 < t1

    def steps(row, size, count):
        return sum(jnp.where(row >= float(size * q), 1.0, 0.0) for q in range(1, count))

    def col(row):
        return jnp.sum(jnp.where(t0 == t1, row, 0.0), axis=1, keepdims=True)

    def down(mask, value=1.0):
        return jnp.sum(jnp.where(mask, value, 0.0), axis=0, keepdims=True)

    dead = -1.0 - lane1
    to_chip = steps(place, 2 * per_owner, chips)
    from_chip = steps(lane1, cap, chips)
    key = jnp.where(live_row, place, dead)
    pair = jnp.where(live_row, from_chip * chips + to_chip, dead)
    dest = jnp.where(live_row, to_chip, dead)
    key_col, pair_col, dest_col, from_col = col(key), col(pair), col(dest), col(from_chip)
    same = key_col == key
    pos = down((pair_col == pair) & before)
    copies = down(same & before)
    first = jnp.where(live_row & (copies == 0.0), 1.0, 0.0)
    first_col = col(first) > 0
    order = down(first_col & (dest_col == dest) & before)
    rank = down(same & first_col, col(order))
    pos_col, copies_col, rank_col = col(pos), col(copies), col(rank)
    mine = dest_col == chip
    hit = mine & (rank_col == lane)
    loc = jnp.where(hit, from_col * cap + pos_col - zero_slab, 0.0)

    def put(row, value):
        tab_ref[row:row + 1, :] = value.astype(jnp.int32)

    for j in range(most):
        put(j, down(copies_col == float(j), loc) + zero_slab)
    put(most, down(hit & first_col, col(place) - 2 * per_owner * chip))
    slot_col = t0.astype(f32)[:, 0:1] - cap * chip
    for q in range(chips):
        put(most + 1 + q, down((from_col == chip) & (dest_col == float(q)) & (pos_col == lane), slot_col))

    def top(row):
        return jnp.max(jnp.where(live_row, row, 0.0), axis=1, keepdims=True)

    crossing = jnp.where(to_chip == from_chip, 0.0, pos + 1.0)
    sizes = (top(rank + 1.0), top(copies + 1.0), top(crossing))
    which = jnp.zeros((1, 1), f32)
    for limits in variants[:-1]:
        over = sum(jnp.where(size > float(limit), 1.0, 0.0) for size, limit in zip(sizes, limits))
        which = which + jnp.where(over > 0, 1.0, 0.0)
    put(most + 1 + chips, jnp.broadcast_to(which, (1, 128)))
    return place_mu


def prep_kernel(
    n, variants, pairs_hbm, counts_hbm, owned_hbm, occ_hbm, blk_hbm, tab_ref, all_ref,
    pairs_ref, counts_ref, owned_ref,
    blk, mscr, msnd, mall, occ_all, lhs, hsnd, b_sem, i_sem, m_s, m_r, o_s, o_r, h_s, h_r,
):
    me = lax.axis_index("ao")
    core = lax.rem(me, 2)
    mate = me + 1 - 2 * core
    slots, deep = blk.shape[0], blk.shape[1]
    per_owner = owned_ref.shape[1]
    rows = occ_hbm.shape[0]
    occupied = rows // per_owner
    barrier = pltpu.get_barrier_semaphore()
    for k in range(1, n):
        pl.semaphore_signal(barrier, inc=1, device_id={"ao": lax.rem(me + k, n)}, device_id_type=MESH)
    reads = [pltpu.make_async_copy(blk_hbm.at[s], blk.at[s], b_sem.at[s]) for s in range(slots)]
    own_occ = occ_all.at[me]
    inputs = [
        pltpu.make_async_copy(src, dst, i_sem.at[i]) for i, (src, dst) in enumerate((
            (pairs_hbm, pairs_ref), (counts_hbm, counts_ref), (owned_hbm, owned_ref), (occ_hbm, own_occ),
        ))
    ]
    for copy in inputs + reads:
        copy.start()
    for copy in inputs:
        copy.wait()
    mscr[...] = jnp.zeros(mscr.shape, jnp.int32)
    mscr[0:2, 0:slots] = pairs_ref[...]
    mscr[2:3, 0:slots] = jnp.where(iota2((1, slots), 1) < counts_ref[...], 1, 0)
    mscr[3:4, 0:per_owner] = owned_ref[...]
    meta = mscr[...]
    by_slot, by_owner = pltpu.roll(meta, me * slots, 1), pltpu.roll(meta, me * per_owner, 1)
    meta = jnp.where(iota2(meta.shape, 0) == 3, by_owner, by_slot)
    msnd[...] = meta
    mall[me] = meta
    with jax.named_scope("barrier"):
        pl.semaphore_wait(barrier, n - 1)
    sent = []
    for k in range(1, n):
        to = {"ao": lax.rem(me + k, n)}
        for src, dst, ss, rs in ((msnd, mall, m_s, m_r), (own_occ, occ_all, o_s, o_r)):
            copy = pltpu.make_async_remote_copy(
                src_ref=src, dst_ref=dst.at[me], send_sem=ss.at[k], recv_sem=rs.at[k],
                device_id=to, device_id_type=MESH,
            )
            copy.start()
            sent.append(copy)
    with jax.named_scope("meta_wait"):
        for copy in sent:
            copy.wait_recv()
    flat = mall[0]
    for r in range(1, n):
        flat = flat + mall[r]
    chip = (me // 2).astype(f32)
    with jax.named_scope("tables"):
        place_mu = make_tables(n, slots, per_owner, chip, variants, flat, tab_ref)

    pair_rows = 2 * occupied * slots
    r0, r1 = iota2((pair_rows, 128), 0), iota2((pair_rows, 128), 1)
    mine = r1 == me * slots + r0 // (2 * occupied)
    want = jnp.sum(jnp.where(mine, place_mu, 0.0), axis=1, keepdims=True) * occupied
    wide = (pair_rows, n * rows)
    want = want + (lax.rem(r0, occupied)).astype(f32)[:, 0:1]
    pick = jnp.where(iota2(wide, 1).astype(f32) == want, 1.0, 0.0).astype(bf16)
    occ = occ_all[...].reshape(n * rows, 128)
    picked = jnp.dot(pick, occ, preferred_element_type=f32)
    upper = lax.rem(r0 // occupied, 2) == 0
    lhs[:, 0:128] = jnp.where(upper, picked, 0.0).astype(bf16)
    lhs[:, 128:256] = jnp.where(upper, 0.0, picked).astype(bf16)

    group = 2 * occupied
    halves = deep // 4
    passed = []
    for s in range(slots):
        with jax.named_scope("read_wait"):
            reads[s].wait()
        left = lhs[s * group:(s + 1) * group, :]

        def product(q):
            right = blk[s, pl.ds(2 * q, 2)].reshape(256, 128)
            return jnp.dot(left, right, preferred_element_type=f32).astype(bf16)

        def out_rows(q):
            return pl.ds(pl.multiple_of(q * group, group), group)

        @pl.loop(0, halves, unroll=8)
        def _(q):
            hsnd[s, out_rows(q), :] = product((1 - core) * halves + q)

        copy = pltpu.make_async_remote_copy(
            src_ref=hsnd.at[s], dst_ref=all_ref.at[core * slots + s], send_sem=h_s.at[s], recv_sem=h_r.at[s],
            device_id={"ao": mate}, device_id_type=MESH,
        )
        copy.start()
        passed.append(copy)

        @pl.loop(0, halves, unroll=8)
        def _(q):
            all_ref[core * slots + s, out_rows(q), :] = product(core * halves + q)

    with jax.named_scope("end_wait"):
        for copy in passed:
            copy.wait()
    for copy in sent:
        copy.wait_send()


def prepare(n, variants, pairs, counts, owned, occ, blocks):
    slots, deep, _, width = blocks.shape
    per_owner, occupied, _ = occ.shape
    rows = per_owner * occupied
    span = deep * occupied // 2
    dma, vm = pltpu.SemaphoreType.DMA, pltpu.VMEM
    whole = pl.BlockSpec(memory_space=pltpu.VMEM)
    return pl.pallas_call(
        functools.partial(prep_kernel, n, variants),
        out_shape=(
            jax.ShapeDtypeStruct((TAB_ROWS, 128), jnp.int32),
            jax.ShapeDtypeStruct((2 * slots, span, width), bf16),
        ),
        in_specs=[pl.BlockSpec(memory_space=pl.ANY)] * 5,
        out_specs=(whole, whole),
        scratch_shapes=[
            vm((2, slots), jnp.int32), vm((1, 1), jnp.int32), vm((1, per_owner), jnp.int32),
            vm(blocks.shape, bf16),
            vm((8, 128), jnp.int32), vm((8, 128), jnp.int32), vm((n, 8, 128), jnp.int32),
            vm((n, rows, width), bf16),
            vm((2 * occupied * slots, 2 * width), bf16),
            vm((slots, span, width), bf16),
            dma((slots,)), dma((4,)), dma((n,)), dma((n,)), dma((n,)), dma((n,)), dma((slots,)), dma((slots,)),
        ],
        compiler_params=pltpu.CompilerParams(
            collective_id=0, has_side_effects=True, vmem_limit_bytes=62 * 1024 * 1024,
        ),
    )(pairs.T, counts.reshape(1, 1), owned.reshape(1, per_owner), occ.reshape(rows, width), blocks)


def main_kernel(n, nz, kept, depth_j, cross, tab_ref, all_ref, vir_hbm, out_ref, *refs):
    (vir_both, vir, snd, rows, part, rx, ry, tx, ty, vir_sem, vir_s, vir_r, a_s, a_r,
     up_s, up_r, dn_s, dn_r, x_s, x_r, y_s, y_r) = refs[:22]
    rcv = refs[22:]
    me, z = lax.axis_index("ao"), lax.axis_index("aux")
    core, chip = lax.rem(me, 2), me // 2
    cx, cy = lax.rem(chip, 2), chip // 2
    mate = me + 1 - 2 * core
    xmate = me + 2 - 4 * cx
    ymate = me + 4 - 8 * cy
    dmate = xmate + 4 - 8 * cy
    others = (xmate, ymate, dmate)
    cap, span, width = all_ref.shape
    per_owner = vir_hbm.shape[0]
    most = n * CAP
    zero_slab = n // 2 * cap
    step = span // CHUNKS
    mid = step // 2

    barrier = pltpu.get_barrier_semaphore()
    for to in (mate,) + others:
        pl.semaphore_signal(barrier, inc=1, device_id={"ao": to}, device_id_type=MESH)
    for k in range(1, nz):
        pl.semaphore_signal(barrier, inc=1, device_id={"aux": lax.rem(z + k, nz)}, device_id_type=MESH)
    own_vir = vir_both.at[pl.ds(core * per_owner, per_owner)]
    vir_copy = pltpu.make_async_copy(vir_hbm, own_vir, vir_sem)
    vir_copy.start()

    with jax.named_scope("pack"):
      for d, to in enumerate(others):
        for j in range(cross):
            snd[d, j] = all_ref[tab_ref[most + 1 + to // 2, j]]
    for j in range(cap):
        slab = all_ref[tab_ref[most + 1 + chip, j]]
        for c in range(CHUNKS):
            rcv[c][chip * cap + j] = slab[c * step:(c + 1) * step]
    for c in range(CHUNKS):
        rcv[c][zero_slab] = jnp.zeros((step, width), bf16)
    with jax.named_scope("barrier2"):
        pl.semaphore_wait(barrier, 1 + len(others) + nz - 1)

    def remote(src, dst, ss, rs, to):
        copy = pltpu.make_async_remote_copy(
            src_ref=src, dst_ref=dst, send_sem=ss, recv_sem=rs, device_id={"ao": to}, device_id_type=MESH,
        )
        copy.start()
        return copy

    a_copies = []
    for c in range(CHUNKS):
        at = pl.ds(chip * cap, cross)
        a_copies.append([
            remote(snd.at[d, :, pl.ds(c * step, step), :], rcv[c].at[at], a_s.at[c, d], a_r.at[c, d], to)
            for d, to in enumerate(others)
        ])
    with jax.named_scope("vir_wait"):
        vir_copy.wait()
    vir_pass = remote(own_vir, own_vir, vir_s, vir_r, mate)

    def z_copy(c, d, up):
        src = z - d if up else z + d
        return pltpu.make_async_remote_copy(
            src_ref=rows.at[c, src], dst_ref=rows.at[c, src],
            send_sem=(up_s if up else dn_s).at[c, d], recv_sem=(up_r if up else dn_r).at[c, d],
            device_id={"aux": z + 1 if up else z - 1}, device_id_type=MESH,
        )

    def z_send(c, d):
        @pl.when((z - d >= 0) & (z + 1 < nz))
        def _():
            z_copy(c, d, True).start()

        @pl.when((z + d < nz) & (z >= 1))
        def _():
            z_copy(c, d, False).start()

    def z_recv(c, d, up):
        src = z - d if up else z + d
        return pltpu.make_async_remote_copy(
            src_ref=rows.at[c, src], dst_ref=rows.at[c, src],
            send_sem=(up_s if up else dn_s).at[c, d - 1], recv_sem=(up_r if up else dn_r).at[c, d - 1],
            device_id={"aux": z - 1 if up else z + 1}, device_id_type=MESH,
        )

    def stage_a(c):
        for copy in a_copies[c]:
            copy.wait_recv()

        @pl.loop(0, kept)
        def _(k):
            acc = rcv[c][tab_ref[0, k]].astype(f32)
            for j in range(1, depth_j):
                acc = acc + rcv[c][tab_ref[j, k]].astype(f32)
            rows[c, z, :, pl.ds(pl.multiple_of(k * width, width), width)] = acc.astype(bf16)

        z_send(c, 0)

    def stage_b(c, d):
        @pl.when(z - d >= 0)
        def _():
            z_recv(c, d, True).wait_recv()

        @pl.when(z + d < nz)
        def _():
            z_recv(c, d, False).wait_recv()

        if d < nz - 1:
            z_send(c, d)

    x_copies, y_copies = {}, {}
    tile = 256
    depth = rows.shape[-1]
    piece = 16

    def stage_v():
        vir_pass.wait_recv()

        @pl.loop(0, width // piece)
        def _(i):
            at = pl.ds(pl.multiple_of(i * piece, piece), piece)
            for k in range(kept):
                to = pl.ds(pl.multiple_of(k * width + i * piece, piece), piece)
                vir[to, :] = vir_both[tab_ref[most, k], at, :]

    lo, hi = pl.ds(0, mid), pl.ds(mid, mid)

    def stage_m(c):
        @pl.loop(0, vir.shape[1] // tile)
        def _(j):
            cols = pl.ds(pl.multiple_of(j * tile, tile), tile)
            left = rows[c].reshape(nz * step, depth)
            got = jnp.dot(left, vir[:, cols], preferred_element_type=f32)
            part[c, :, :, cols] = got.astype(bf16).reshape(nz, step, tile)

        far = 2 * (1 - cy) + 1 - cx
        x_copies[c] = [
            remote(part.at[c, far, lo], rx.at[c, 0], x_s.at[c, 0], x_r.at[c, 0], xmate),
            remote(part.at[c, far, hi], ry.at[c, 0], y_s.at[c, 0], y_r.at[c, 0], ymate),
            remote(part.at[c, 2 * cy + 1 - cx, lo], rx.at[c, 1], x_s.at[c, 1], x_r.at[c, 1], xmate),
            remote(part.at[c, 2 * (1 - cy) + cx, hi], ry.at[c, 1], y_s.at[c, 1], y_r.at[c, 1], ymate),
        ]

    def add2(a, b):
        return (a.astype(f32) + b.astype(f32)).astype(bf16)

    def stage_x(c):
        for copy in x_copies[c][:2]:
            copy.wait_recv()
        tx[c] = add2(part[c, 2 * (1 - cy) + cx, :mid], rx[c, 0])
        ty[c] = add2(part[c, 2 * cy + 1 - cx, mid:], ry[c, 0])
        y_copies[c] = [
            remote(tx.at[c], rx.at[c, 2], y_s.at[c, 2], y_r.at[c, 2], ymate),
            remote(ty.at[c], ry.at[c, 2], x_s.at[c, 2], x_r.at[c, 2], xmate),
        ]

    def stage_y(c):
        for copy in x_copies[c][2:] + y_copies[c]:
            copy.wait_recv()
        own = part[c, chip]
        top = own[:mid].astype(f32) + rx[c, 1].astype(f32) + rx[c, 2].astype(f32)
        low = own[mid:].astype(f32) + ry[c, 1].astype(f32) + ry[c, 2].astype(f32)
        out_ref[c * step:c * step + mid, :] = top.astype(bf16)
        out_ref[c * step + mid:(c + 1) * step, :] = low.astype(bf16)

    plan = (
        "A0 A1 B01 B02", "A2 V B03 M0", "B11 B12 A3 X0", "B13 M1 B21 B22", "X1 Y0 B23 M2",
        "B31 B32 X2 Y1", "B33 M3 X3", "Y2 Y3",
    )
    run = {"A": stage_a, "B": stage_b, "M": stage_m, "X": stage_x, "Y": stage_y, "V": stage_v}
    for item in [name for row in plan for name in row.split()]:
        with jax.named_scope(item):
            run[item[0]](*[int(v) for v in item[1:]])

    vir_pass.wait_send()
    for c in range(CHUNKS):
        for copy in a_copies[c] + x_copies[c] + y_copies[c]:
            copy.wait_send()
        for d in range(nz - 1):
            @pl.when((z - d >= 0) & (z + 1 < nz))
            def _():
                z_copy(c, d, True).wait_send()

            @pl.when((z + d < nz) & (z >= 1))
            def _():
                z_copy(c, d, False).wait_send()


def fused(n, nz, sizes, call_id, tab, slabs, vir3):
    kept, depth_j, cross = sizes
    cap, span, width = slabs.shape
    per_owner, _, columns = vir3.shape
    step = span // CHUNKS
    dma, vm = pltpu.SemaphoreType.DMA, pltpu.VMEM
    return pl.pallas_call(
        functools.partial(main_kernel, n, nz, kept, depth_j, cross),
        out_shape=jax.ShapeDtypeStruct((span, columns), bf16),
        in_specs=[
            pl.BlockSpec(memory_space=pltpu.SMEM),
            pl.BlockSpec(memory_space=pltpu.VMEM),
            pl.BlockSpec(memory_space=pl.ANY),
        ],
        out_specs=pl.BlockSpec(memory_space=pltpu.VMEM),
        scratch_shapes=[
            vm((2 * per_owner, width, columns), bf16),
            vm((kept * width, columns), bf16),
            vm((3, cross, span, width), bf16),
            vm((CHUNKS, nz, step, kept * width), bf16),
            vm((CHUNKS, nz, step, columns), bf16),
            vm((CHUNKS, 3, step // 2, columns), bf16),
            vm((CHUNKS, 3, step // 2, columns), bf16),
            vm((CHUNKS, step // 2, columns), bf16),
            vm((CHUNKS, step // 2, columns), bf16),
            dma, dma, dma,
            dma((CHUNKS, 3)), dma((CHUNKS, 3)),
            dma((CHUNKS, nz)), dma((CHUNKS, nz)), dma((CHUNKS, nz)), dma((CHUNKS, nz)),
            dma((CHUNKS, 3)), dma((CHUNKS, 3)), dma((CHUNKS, 3)), dma((CHUNKS, 3)),
        ] + [vm((n // 2 * cap + 1, step, width), bf16)] * CHUNKS,
        compiler_params=pltpu.CompilerParams(
            collective_id=call_id, has_side_effects=True, vmem_limit_bytes=62 * 1024 * 1024,
        ),
    )(tab, slabs, vir3)


def per_device(blocks, pairs, counts, owned_blocks, occ_coef, vir_coef):
    groups, nz = lax.axis_size("ao"), lax.axis_size("aux")
    slots, _, _, width = blocks.shape
    per_owner, occupied, _ = occ_coef.shape
    variants = ((10, 4, 6), (12, 6, 9), (2 * per_owner, groups * CAP, 2 * slots))
    tab, slabs = prepare(groups, variants, pairs, counts, owned_blocks, occ_coef, blocks)
    vir3 = vir_coef.reshape(per_owner, width, vir_coef.shape[1])
    which = tab[groups * CAP + 1 + groups // 2, 0]
    out = lax.switch(
        which, [functools.partial(fused, groups, nz, v, 1 + i) for i, v in enumerate(variants)], tab, slabs, vir3,
    )
    return out.reshape(-1, occupied, vir_coef.shape[1])


def per_device_general(blocks, pairs, counts, owned_blocks, occ_coef, vir_coef):
    groups = lax.axis_size("ao")
    own_index = lax.axis_index("ao")
    slot_count = blocks.shape[0]
    aux_depth = blocks.shape[1]
    block_width = blocks.shape[3]
    occupied = occ_coef.shape[1]
    all_pairs, all_counts, all_owned = (
        lax.all_gather(pairs, "ao", axis=0, tiled=True),
        lax.all_gather(counts, "ao", axis=0, tiled=True),
        lax.all_gather(owned_blocks, "ao", axis=0, tiled=True),
    )
    occ_all = lax.all_gather(occ_coef, "ao", axis=0, tiled=True)
    per_owner = all_owned.shape[0] // groups
    slot_ids = jnp.arange(slot_count, dtype=jnp.int32)
    in_use = slot_ids < counts[0]
    occ_pick = occ_all[block_place(pairs[:, 0], all_owned)]
    slab_values = jnp.einsum("sim,spmn->spin", occ_pick, blocks, preferred_element_type=jnp.float32)
    slab_values = jnp.where(in_use[:, None, None, None], slab_values, 0.0).astype(jnp.bfloat16)
    flat_slabs = slab_values.reshape(slot_count, aux_depth * occupied, block_width)
    place_all = block_place(all_pairs[:, 1], all_owned).reshape(groups, slot_count)
    owner_all = place_all // per_owner
    local_all = place_all % per_owner
    live_all = slot_ids[None, :] < all_counts[:, None]
    mine_all = live_all & (owner_all == own_index)
    local_ids = jnp.arange(per_owner, dtype=jnp.int32)
    slabs_got = lax.all_gather(flat_slabs, "ao", axis=0, tiled=True)
    assign = (
        mine_all.reshape(-1)[None, :] & (local_all.reshape(-1)[None, :] == local_ids[:, None])
    ).astype(jnp.bfloat16)
    summed = jnp.einsum("lt,tqm->qlm", assign, slabs_got, preferred_element_type=jnp.float32)
    rows_local = summed.reshape(summed.shape[0], per_owner * block_width).astype(jnp.bfloat16)
    rows_whole = lax.all_gather(rows_local, "aux", axis=0, tiled=True)
    share = rows_whole.shape[0] // groups
    result = lax.psum_scatter(
        jnp.dot(rows_whole, vir_coef, preferred_element_type=jnp.float32).astype(jnp.bfloat16),
        "ao",
        scatter_dimension=0,
        tiled=True,
    )
    return result.reshape(share // occupied, occupied, vir_coef.shape[1])


def solution(mesh):
    in_specs = (
        P("ao", "aux", None, None),
        P("ao", None),
        P("ao"),
        P("ao"),
        P("ao", None, None),
        P("ao", "aux"),
    )
    out_specs = P("ao", None, "aux")
    small = mesh.shape["ao"] == 8 and mesh.shape["aux"] == 4
    body = per_device if small else per_device_general
    return jax.shard_map(body, mesh=mesh, in_specs=in_specs, out_specs=out_specs, check_vma=False)
```

```python
import functools

import jax
import jax.numpy as jnp
from jax import lax
from jax.experimental import pallas as pl
from jax.experimental.pallas import tpu as pltpu
from jax.sharding import PartitionSpec as P

MESH = pl.DeviceIdType.MESH
CAP = 3
CHUNKS = (1,) * 8
VARIANTS = ((8, 4, 6), (10, 4, 6), (10, 4, 9), (12, 6, 9))
TAB_ROWS = 32
f32 = jnp.float32
bf16 = jnp.bfloat16


def block_place(block_ids, owned_all):
    hits = block_ids[..., None] == owned_all
    positions = jnp.arange(owned_all.shape[0], dtype=jnp.int32)
    return jnp.sum(jnp.where(hits, positions, 0), axis=-1)


def iota2(shape, axis):
    return lax.broadcasted_iota(jnp.int32, shape, axis)


def make_tables(n, slots, per_owner, chip, variants, flat, tab_ref, which_ref):
    total, owned, cap = n * slots, n * per_owner, 2 * slots
    chips, most, zero_slab = n // 2, n * CAP, n * slots
    flat = flat.astype(f32)
    nu_row, live_row, own_row = flat[1:2], flat[2:3] > 0, flat[3:4]
    o0, o1 = iota2((owned, 128), 0), iota2((owned, 128), 1)
    own_col = jnp.sum(jnp.where(o0 == o1, own_row, 0.0), axis=1, keepdims=True)
    place_mu, place = (
        jnp.sum(jnp.where(own_col == row, o0.astype(f32), 0.0), axis=0, keepdims=True) for row in (flat[0:1], nu_row)
    )
    t0, t1 = iota2((total, 128), 0), iota2((total, 128), 1)
    lane = t1.astype(f32)
    lane1 = lane[0:1]
    before = t0 < t1

    def steps(row, size, count):
        return sum(jnp.where(row >= float(size * q), 1.0, 0.0) for q in range(1, count))

    def col(row):
        return jnp.sum(jnp.where(t0 == t1, row, 0.0), axis=1, keepdims=True)

    def down(mask, value=1.0):
        return jnp.sum(jnp.where(mask, value, 0.0), axis=0, keepdims=True)

    dead = -1.0 - lane1
    to_chip = steps(place, 2 * per_owner, chips)
    from_chip = steps(lane1, cap, chips)
    key = jnp.where(live_row, place, dead)
    pair = jnp.where(live_row, from_chip * chips + to_chip, dead)
    dest = jnp.where(live_row, to_chip, dead)
    key_col, pair_col, dest_col, from_col = col(key), col(pair), col(dest), col(from_chip)
    same = key_col == key
    pos = down((pair_col == pair) & before)
    copies = down(same & before)
    first = jnp.where(live_row & (copies == 0.0), 1.0, 0.0)
    first_col = col(first) > 0
    order = down(first_col & (dest_col == dest) & before)
    rank = down(same & first_col, col(order))
    pos_col, copies_col, rank_col = col(pos), col(copies), col(rank)
    mine = dest_col == chip
    hit = mine & (rank_col == lane)
    loc = jnp.where(hit, from_col * cap + pos_col - zero_slab, 0.0)

    def put(row, value):
        tab_ref[row:row + 1, :] = value.astype(jnp.int32)

    for j in range(most):
        put(j, down(copies_col == float(j), loc) + zero_slab)
    put(most, down(hit & first_col, col(place) - 2 * per_owner * chip))
    slot_col = t0.astype(f32)[:, 0:1] - cap * chip
    for q in range(chips):
        put(most + 1 + q, down((from_col == chip) & (dest_col == float(q)) & (pos_col == lane), slot_col))

    def top(row):
        return jnp.max(jnp.where(live_row, row, 0.0), axis=1, keepdims=True)

    crossing = jnp.where(to_chip == from_chip, 0.0, pos + 1.0)
    sizes = (top(rank + 1.0), top(copies + 1.0), top(crossing))
    which = jnp.zeros((1, 1), f32)
    for limits in variants[:-1]:
        over = sum(jnp.where(size > float(limit), 1.0, 0.0) for size, limit in zip(sizes, limits))
        which = which + jnp.where(over > 0, 1.0, 0.0)
    which_ref[...] = which.astype(jnp.int32)
    return place_mu


def prep_kernel(
    n, variants, pairs_hbm, counts_hbm, owned_hbm, occ_hbm, tab_ref, lhs, which_ref,
    pairs_ref, counts_ref, owned_ref, mscr, msnd, mall, occ_all, i_sem, m_s, m_r, o_s, o_r,
):
    me = lax.axis_index("ao")
    slots = pairs_ref.shape[1]
    per_owner = owned_ref.shape[1]
    rows = occ_hbm.shape[0]
    occupied = rows // per_owner
    barrier = pltpu.get_barrier_semaphore()
    for k in range(1, n):
        pl.semaphore_signal(barrier, inc=1, device_id={"ao": lax.rem(me + k, n)}, device_id_type=MESH)
    own_occ = occ_all.at[me]
    inputs = [
        pltpu.make_async_copy(src, dst, i_sem.at[i]) for i, (src, dst) in enumerate((
            (pairs_hbm, pairs_ref), (counts_hbm, counts_ref), (owned_hbm, owned_ref), (occ_hbm, own_occ),
        ))
    ]
    for copy in inputs:
        copy.start()
    for copy in inputs:
        copy.wait()
    mscr[...] = jnp.zeros(mscr.shape, jnp.int32)
    mscr[0:2, 0:slots] = pairs_ref[...]
    mscr[2:3, 0:slots] = jnp.where(iota2((1, slots), 1) < counts_ref[...], 1, 0)
    mscr[3:4, 0:per_owner] = owned_ref[...]
    meta = mscr[...]
    by_slot, by_owner = pltpu.roll(meta, me * slots, 1), pltpu.roll(meta, me * per_owner, 1)
    meta = jnp.where(iota2(meta.shape, 0) == 3, by_owner, by_slot)
    msnd[...] = meta
    mall[me] = meta
    with jax.named_scope("barrier"):
        pl.semaphore_wait(barrier, n - 1)
    sent = []
    for k in range(1, n):
        to = {"ao": lax.rem(me + k, n)}
        for src, dst, ss, rs in ((msnd, mall, m_s, m_r), (own_occ, occ_all, o_s, o_r)):
            copy = pltpu.make_async_remote_copy(
                src_ref=src, dst_ref=dst.at[me], send_sem=ss.at[k], recv_sem=rs.at[k],
                device_id=to, device_id_type=MESH,
            )
            copy.start()
            sent.append(copy)
    with jax.named_scope("meta_wait"):
        for copy in sent:
            copy.wait_recv()
    flat = mall[0]
    for r in range(1, n):
        flat = flat + mall[r]
    chip = (me // 2).astype(f32)
    with jax.named_scope("tables"):
        place_mu = make_tables(n, slots, per_owner, chip, variants, flat, tab_ref, which_ref)

    pair_rows = 2 * occupied * slots
    r0, r1 = iota2((pair_rows, 128), 0), iota2((pair_rows, 128), 1)
    mine = r1 == me * slots + r0 // (2 * occupied)
    want = jnp.sum(jnp.where(mine, place_mu, 0.0), axis=1, keepdims=True) * occupied
    wide = (pair_rows, n * rows)
    want = want + (lax.rem(r0, occupied)).astype(f32)[:, 0:1]
    pick = jnp.where(iota2(wide, 1).astype(f32) == want, 1.0, 0.0).astype(bf16)
    occ = occ_all[...].reshape(n * rows, 128)
    picked = jnp.dot(pick, occ, preferred_element_type=f32)
    upper = lax.rem(r0 // occupied, 2) == 0
    lhs[:, 0:128] = jnp.where(upper, picked, 0.0).astype(bf16)
    lhs[:, 128:256] = jnp.where(upper, 0.0, picked).astype(bf16)

    for copy in sent:
        copy.wait_send()


def prepare(n, variants, pairs, counts, owned, occ):
    slots = pairs.shape[0]
    per_owner, occupied, width = occ.shape
    rows = per_owner * occupied
    dma, vm = pltpu.SemaphoreType.DMA, pltpu.VMEM
    whole = pl.BlockSpec(memory_space=pltpu.VMEM)
    return pl.pallas_call(
        functools.partial(prep_kernel, n, variants),
        out_shape=(
            jax.ShapeDtypeStruct((TAB_ROWS, 128), jnp.int32),
            jax.ShapeDtypeStruct((2 * occupied * slots, 2 * width), bf16),
            jax.ShapeDtypeStruct((1, 1), jnp.int32),
        ),
        in_specs=[pl.BlockSpec(memory_space=pl.ANY)] * 4,
        out_specs=(whole,) * 3,
        scratch_shapes=[
            vm((2, slots), jnp.int32), vm((1, 1), jnp.int32), vm((1, per_owner), jnp.int32),
            vm((8, 128), jnp.int32), vm((8, 128), jnp.int32), vm((n, 8, 128), jnp.int32),
            vm((n, rows, width), bf16),
            dma((4,)), dma((n,)), dma((n,)), dma((n,)), dma((n,)),
        ],
        compiler_params=pltpu.CompilerParams(
            collective_id=0, has_side_effects=True, vmem_limit_bytes=62 * 1024 * 1024,
        ),
    )(pairs.T, counts.reshape(1, 1), owned.reshape(1, per_owner), occ.reshape(rows, width))


def cuts(span):
    out, at = [], 0
    for part in CHUNKS:
        out.append((at, part * span // 8))
        at += part * span // 8
    return out


def make_plan(count):
    out = ["H0"]
    for c in range(1, count + 1):
        out += ["H%d" % c] + ["W"] * (c == count - 1) + ["P%d" % (c - 1)]
    out += ["A0", "A1", "F0", "A2", "F1", "V", "A3", "F2", "M0"]
    for c in range(count):
        out += ["A%d" % (c + 4), "F%d" % (c + 3), "M%d" % (c + 1), "X%d" % c, "Y%d" % (c - 1)]
        out += ["S%d" % (c - 2), "T%d" % (c - 3)]
    out += ["Y%d" % (count - 1)]
    out += ["S%d" % c for c in range(count - 2, count)] + ["T%d" % c for c in range(count - 3, count)]
    return [name for name in out if len(name) == 1 or 0 <= int(name[1:]) < count]


def main_kernel(n, nz, kept, depth_j, cross, tab_ref, lhs_ref, blk_hbm, vir_hbm, out_hbm, out_ref, out_sem, *refs):
    (vir_both, vir, blk, hsnd, snd, rows, part, rx, ry, tx, ty, vir_sem, vir_s, vir_r, b_sem, h_s, h_r, a_s, a_r,
     up_s, up_r, dn_s, dn_r, x_s, x_r, y_s, y_r) = refs[:27]
    pieces = refs[27:]
    count = len(pieces) // 2
    slab, rcv = pieces[:count], pieces[count:]
    me, z = lax.axis_index("ao"), lax.axis_index("aux")
    core, chip = lax.rem(me, 2), me // 2
    cx, cy = lax.rem(chip, 2), chip // 2
    mate = me + 1 - 2 * core
    xmate = me + 2 - 4 * cx
    ymate = me + 4 - 8 * cy
    others = (xmate, ymate, xmate + 4 - 8 * cy)
    slots, span, width = hsnd.shape
    cap = 2 * slots
    deep = blk.shape[1] // 2
    occupied = span // deep
    group = 2 * occupied
    per_owner = vir_hbm.shape[0]
    most = n * CAP
    zero_slab = n // 2 * cap
    chunks = cuts(span)

    barrier = pltpu.get_barrier_semaphore()
    for to in (mate,) + others:
        pl.semaphore_signal(barrier, inc=1, device_id={"ao": to}, device_id_type=MESH)

    for d in (1, 2):
        @pl.when(z + d < nz)
        def _():
            pl.semaphore_signal(barrier, inc=1, device_id={"aux": z + d}, device_id_type=MESH)

        @pl.when(z - d >= 0)
        def _():
            pl.semaphore_signal(barrier, inc=1, device_id={"aux": z - d}, device_id_type=MESH)

    reads = []
    for c, (at, step) in enumerate(chunks):
        pair = []
        for i, half in enumerate((1 - core, core)):
            these = pl.ds(half * deep + at // occupied, step // occupied)
            pair.append(pltpu.make_async_copy(blk_hbm.at[:, these], blk.at[:, these], b_sem.at[c, i]))
            pair[-1].start()
        reads.append(pair)
    own_vir = vir_both.at[pl.ds(core * per_owner, per_owner)]
    vir_copy = pltpu.make_async_copy(vir_hbm, own_vir, vir_sem)
    vir_copy.start()

    def remote(src, dst, ss, rs, to):
        copy = pltpu.make_async_remote_copy(
            src_ref=src, dst_ref=dst, send_sem=ss, recv_sem=rs, device_id={"ao": to}, device_id_type=MESH,
        )
        copy.start()
        return copy

    h_copies, a_copies, vir_pass = {}, {}, []

    def stage_h(c):
        at, step = chunks[c]

        def product(s, half, q):
            right = blk[s, pl.ds(half * deep + at // occupied + 2 * q, 2)].reshape(2 * width, width)
            left = lhs_ref[pl.ds(pl.multiple_of(s * group, group), group), :]
            return jnp.dot(left, right, preferred_element_type=f32).astype(bf16)

        for copy in reads[c]:
            copy.wait()

        @pl.loop(0, slots, unroll=3)
        def _(s):
            for q in range(step // group):
                hsnd[s, at + q * group:at + (q + 1) * group, :] = product(s, 1 - core, q)
                slab[c][core * slots + s, q * group:(q + 1) * group, :] = product(s, core, q)

        if c == 0:
            for w in range(2):
                @pl.when((z >= 1) & (z + 1 < nz) if w else (z < 1) | (z + 1 >= nz))
                def _():
                    pl.semaphore_wait(barrier, 6 + w)
        h_copies[c] = remote(
            hsnd.at[:, pl.ds(at, step), :], slab[c].at[pl.ds(core * slots, slots)], h_s.at[c], h_r.at[c], mate,
        )

    def stage_p(c):
        at, step = chunks[c]
        h_copies[c].wait_recv()
        for d, to in enumerate(others):
            for j in range(cross):
                snd[d, j, at:at + step, :] = slab[c][tab_ref[most + 1 + to // 2, j]]
        a_copies[c] = [
            remote(snd.at[d, :, pl.ds(at, step), :], rcv[c].at[pl.ds(chip * cap, cross)], a_s.at[c, d], a_r.at[c, d], to)
            for d, to in enumerate(others)
        ]
        for j in range(cap):
            rcv[c][chip * cap + j] = slab[c][tab_ref[most + 1 + chip, j]]
        rcv[c][zero_slab] = jnp.zeros((step, width), bf16)

    def stage_w():
        vir_copy.wait()
        vir_pass.append(remote(own_vir, own_vir, vir_s, vir_r, mate))

    def z_copy(c, d, up):
        src = z if d < 3 else z - 2 if up else z + 2
        hop = min(d, 2) if d < 3 else 1
        return pltpu.make_async_remote_copy(
            src_ref=rows.at[src, pl.ds(*chunks[c])], dst_ref=rows.at[src, pl.ds(*chunks[c])],
            send_sem=(up_s if up else dn_s).at[c, d], recv_sem=(up_r if up else dn_r).at[c, d],
            device_id={"aux": z + hop if up else z - hop}, device_id_type=MESH,
        )

    def z_sends(d, up):
        if d < 3:
            return z + d < nz if up else z - d >= 0
        return (z >= 2) & (z + 1 < nz) if up else (z + 2 < nz) & (z >= 1)

    def z_recv(c, d, up):
        src = z - d if up else z + d
        hop = d if d < 3 else 1
        return pltpu.make_async_remote_copy(
            src_ref=rows.at[src, pl.ds(*chunks[c])], dst_ref=rows.at[src, pl.ds(*chunks[c])],
            send_sem=(up_s if up else dn_s).at[c, d], recv_sem=(up_r if up else dn_r).at[c, d],
            device_id={"aux": z - hop if up else z + hop}, device_id_type=MESH,
        )

    def z_start(c, d):
        for up in (True, False):
            @pl.when(z_sends(d, up))
            def _():
                z_copy(c, d, up).start()

    def stage_f(c):
        for up in (True, False):
            @pl.when(z_sends(3, up))
            def _():
                z_recv(c, 2, up).wait_recv()
                z_copy(c, 3, up).start()

    def z_rest(c):
        for d in range(1, nz):
            for up in (True, False):
                here = z - d >= 0 if up else z + d < nz

                @pl.when(here & jnp.logical_not(z_sends(3, up)) if d == 2 else here)
                def _():
                    z_recv(c, d, up).wait_recv()

    def stage_a(c):
        at, step = chunks[c]
        for copy in a_copies[c]:
            copy.wait_recv()

        @pl.loop(0, kept)
        def _(k):
            acc = rcv[c][tab_ref[0, k]].astype(f32)
            for j in range(1, depth_j):
                acc = acc + rcv[c][tab_ref[j, k]].astype(f32)
            rows[z, at:at + step, pl.ds(pl.multiple_of(k * width, width), width)] = acc.astype(bf16)

        z_start(c, 2)
        z_start(c, 1)

    x_copies, y_copies, o_copies = {}, {}, {}
    tile = 256
    depth = rows.shape[-1]
    piece = 16

    def stage_v():
        vir_pass[0].wait_recv()

        @pl.loop(0, width // piece)
        def _(i):
            at = pl.ds(pl.multiple_of(i * piece, piece), piece)
            for k in range(kept):
                to = pl.ds(pl.multiple_of(k * width + i * piece, piece), piece)
                vir[to, :] = vir_both[tab_ref[most, k], at, :]

    def stage_m(c):
        at, step = chunks[c]
        mid = step // 2
        lo, hi, here = pl.ds(at, mid), pl.ds(at + mid, mid), pl.ds(at // 2, mid)

        with jax.named_scope("Z"):
            z_rest(c)

        @pl.loop(0, vir.shape[1] // tile)
        def _(j):
            cols = pl.ds(pl.multiple_of(j * tile, tile), tile)
            left = rows[:, at:at + step, :].reshape(nz * step, depth)
            got = jnp.dot(left, vir[:, cols], preferred_element_type=f32)
            part[:, at:at + step, cols] = got.astype(bf16).reshape(nz, step, tile)

        far = 2 * (1 - cy) + 1 - cx
        x_copies[c] = [
            remote(part.at[far, lo], rx.at[0, here], x_s.at[c, 0], x_r.at[c, 0], xmate),
            remote(part.at[far, hi], ry.at[0, here], y_s.at[c, 0], y_r.at[c, 0], ymate),
            remote(part.at[2 * cy + 1 - cx, lo], rx.at[1, here], x_s.at[c, 1], x_r.at[c, 1], xmate),
            remote(part.at[2 * (1 - cy) + cx, hi], ry.at[1, here], y_s.at[c, 1], y_r.at[c, 1], ymate),
        ]

    def add2(a, b):
        return (a.astype(f32) + b.astype(f32)).astype(bf16)

    def stage_x(c):
        at, step = chunks[c]
        mid = step // 2
        here, there = slice(at // 2, at // 2 + mid), pl.ds(at // 2, mid)
        for copy in x_copies[c][:2]:
            copy.wait_recv()
        tx[here] = add2(part[2 * (1 - cy) + cx, at:at + mid], rx[0, here])
        ty[here] = add2(part[2 * cy + 1 - cx, at + mid:at + step], ry[0, here])
        y_copies[c] = [
            remote(tx.at[there], rx.at[2, there], y_s.at[c, 2], y_r.at[c, 2], ymate),
            remote(ty.at[there], ry.at[2, there], x_s.at[c, 2], x_r.at[c, 2], xmate),
        ]

    def stage_y(c):
        at, step = chunks[c]
        mid = step // 2
        here = slice(at // 2, at // 2 + mid)
        for copy in x_copies[c][2:] + y_copies[c]:
            copy.wait_recv()
        top = part[chip, at:at + mid].astype(f32) + rx[1, here].astype(f32) + rx[2, here].astype(f32)
        low = part[chip, at + mid:at + step].astype(f32) + ry[1, here].astype(f32) + ry[2, here].astype(f32)
        out_ref[at:at + mid, :] = top.astype(bf16)
        out_ref[at + mid:at + step, :] = low.astype(bf16)
        o_copies[c] = pltpu.make_async_copy(out_ref.at[pl.ds(at, step)], out_hbm.at[pl.ds(at, step)], out_sem.at[c])
        o_copies[c].start()

    def stage_s(c):
        for copy in [h_copies[c]] + a_copies[c]:
            copy.wait_send()
        for d in range(1, nz):
            for up in (True, False):
                @pl.when(z_sends(d, up))
                def _():
                    z_copy(c, d, up).wait_send()

    def stage_t(c):
        for copy in x_copies[c] + y_copies[c]:
            copy.wait_send()
        o_copies[c].wait()

    run = {"H": stage_h, "P": stage_p, "W": stage_w, "A": stage_a, "F": stage_f, "M": stage_m, "X": stage_x,
           "Y": stage_y, "V": stage_v, "S": stage_s, "T": stage_t}
    for item in make_plan(count):
        with jax.named_scope(item):
            run[item[0]](*[int(v) for v in item[1:]])
    vir_pass[0].wait_send()


def fused(n, nz, sizes, call_id, tab, lhs, blocks, vir3):
    kept, depth_j, cross = sizes
    slots, deep, _, width = blocks.shape
    per_owner, _, columns = vir3.shape
    span = deep * lhs.shape[0] // slots // 4
    steps = [step for _, step in cuts(span)]
    count, cap = len(steps), 2 * slots
    dma, vm = pltpu.SemaphoreType.DMA, pltpu.VMEM
    anywhere, whole = pl.BlockSpec(memory_space=pl.ANY), pl.BlockSpec(memory_space=pltpu.VMEM)
    return pl.pallas_call(
        functools.partial(main_kernel, n, nz, kept, depth_j, cross),
        out_shape=jax.ShapeDtypeStruct((span, columns), bf16),
        in_specs=[pl.BlockSpec(memory_space=pltpu.SMEM), whole, anywhere, anywhere],
        out_specs=anywhere,
        scratch_shapes=[
            vm((span, columns), bf16), dma((count,)),
            vm((2 * per_owner, width, columns), bf16),
            vm((kept * width, columns), bf16),
            vm(blocks.shape, bf16),
            vm((slots, span, width), bf16),
            vm((3, cross, span, width), bf16),
            vm((nz, span, kept * width), bf16),
            vm((nz, span, columns), bf16),
            vm((3, span // 2, columns), bf16),
            vm((3, span // 2, columns), bf16),
            vm((span // 2, columns), bf16),
            vm((span // 2, columns), bf16),
            dma, dma, dma,
            dma((count, 2)), dma((count,)), dma((count,)),
            dma((count, 3)), dma((count, 3)),
            dma((count, nz)), dma((count, nz)), dma((count, nz)), dma((count, nz)),
            dma((count, 3)), dma((count, 3)), dma((count, 3)), dma((count, 3)),
        ] + [vm((cap, step, width), bf16) for step in steps] + [
            vm((n // 2 * cap + 1, step, width), bf16) for step in steps
        ],
        compiler_params=pltpu.CompilerParams(
            collective_id=call_id, has_side_effects=True, vmem_limit_bytes=62 * 1024 * 1024,
        ),
    )(tab, lhs, blocks, vir3)


def per_device(blocks, pairs, counts, owned_blocks, occ_coef, vir_coef):
    groups, nz = lax.axis_size("ao"), lax.axis_size("aux")
    slots, _, _, width = blocks.shape
    per_owner, occupied, _ = occ_coef.shape
    variants = VARIANTS + ((2 * per_owner, groups * CAP, 2 * slots),)
    tab, lhs, which = prepare(groups, variants, pairs, counts, owned_blocks, occ_coef)
    vir3 = vir_coef.reshape(per_owner, width, vir_coef.shape[1])
    out = lax.switch(
        which.reshape(()), [functools.partial(fused, groups, nz, v, 1 + i) for i, v in enumerate(variants)],
        tab, lhs, blocks, vir3,
    )
    return out.reshape(-1, occupied, vir_coef.shape[1])


def per_device_general(blocks, pairs, counts, owned_blocks, occ_coef, vir_coef):
    groups = lax.axis_size("ao")
    own_index = lax.axis_index("ao")
    slot_count = blocks.shape[0]
    aux_depth = blocks.shape[1]
    block_width = blocks.shape[3]
    occupied = occ_coef.shape[1]
    all_pairs, all_counts, all_owned = (
        lax.all_gather(pairs, "ao", axis=0, tiled=True),
        lax.all_gather(counts, "ao", axis=0, tiled=True),
        lax.all_gather(owned_blocks, "ao", axis=0, tiled=True),
    )
    occ_all = lax.all_gather(occ_coef, "ao", axis=0, tiled=True)
    per_owner = all_owned.shape[0] // groups
    slot_ids = jnp.arange(slot_count, dtype=jnp.int32)
    in_use = slot_ids < counts[0]
    occ_pick = occ_all[block_place(pairs[:, 0], all_owned)]
    slab_values = jnp.einsum("sim,spmn->spin", occ_pick, blocks, preferred_element_type=jnp.float32)
    slab_values = jnp.where(in_use[:, None, None, None], slab_values, 0.0).astype(jnp.bfloat16)
    flat_slabs = slab_values.reshape(slot_count, aux_depth * occupied, block_width)
    place_all = block_place(all_pairs[:, 1], all_owned).reshape(groups, slot_count)
    owner_all = place_all // per_owner
    local_all = place_all % per_owner
    live_all = slot_ids[None, :] < all_counts[:, None]
    mine_all = live_all & (owner_all == own_index)
    local_ids = jnp.arange(per_owner, dtype=jnp.int32)
    slabs_got = lax.all_gather(flat_slabs, "ao", axis=0, tiled=True)
    assign = (
        mine_all.reshape(-1)[None, :] & (local_all.reshape(-1)[None, :] == local_ids[:, None])
    ).astype(jnp.bfloat16)
    summed = jnp.einsum("lt,tqm->qlm", assign, slabs_got, preferred_element_type=jnp.float32)
    rows_local = summed.reshape(summed.shape[0], per_owner * block_width).astype(jnp.bfloat16)
    rows_whole = lax.all_gather(rows_local, "aux", axis=0, tiled=True)
    share = rows_whole.shape[0] // groups
    result = lax.psum_scatter(
        jnp.dot(rows_whole, vir_coef, preferred_element_type=jnp.float32).astype(jnp.bfloat16),
        "ao",
        scatter_dimension=0,
        tiled=True,
    )
    return result.reshape(share // occupied, occupied, vir_coef.shape[1])


def solution(mesh):
    in_specs = (
        P("ao", "aux", None, None),
        P("ao", None),
        P("ao"),
        P("ao"),
        P("ao", None, None),
        P("ao", "aux"),
    )
    out_specs = P("ao", None, "aux")
    small = mesh.shape["ao"] == 8 and mesh.shape["aux"] == 4
    body = per_device if small else per_device_general
    return jax.shard_map(body, mesh=mesh, in_specs=in_specs, out_specs=out_specs, check_vma=False)
```

```python
import functools

import jax
import jax.numpy as jnp
from jax import lax
from jax.experimental import pallas as pl
from jax.experimental.pallas import tpu as pltpu
from jax.sharding import PartitionSpec as P

MESH = pl.DeviceIdType.MESH
CAP = 3
CHUNKS = (1,) * 8
VARIANTS = ((8, 4, 6), (9, 4, 6), (10, 4, 6), (12, 6, 6), (12, 6, 9))
TAB_ROWS = 32
f32 = jnp.float32
bf16 = jnp.bfloat16


def block_place(block_ids, owned_all):
    hits = block_ids[..., None] == owned_all
    positions = jnp.arange(owned_all.shape[0], dtype=jnp.int32)
    return jnp.sum(jnp.where(hits, positions, 0), axis=-1)


def iota2(shape, axis):
    return lax.broadcasted_iota(jnp.int32, shape, axis)


def make_tables(n, slots, per_owner, chip, variants, flat, tab_ref, which_ref):
    total, owned, cap = n * slots, n * per_owner, 2 * slots
    chips, most, zero_slab = n // 2, n * CAP, n * slots
    flat = flat.astype(f32)
    nu_row, live_row, own_row = flat[1:2], flat[2:3] > 0, flat[3:4]
    o0, o1 = iota2((owned, 128), 0), iota2((owned, 128), 1)
    own_col = jnp.sum(jnp.where(o0 == o1, own_row, 0.0), axis=1, keepdims=True)
    place_mu, place = (
        jnp.sum(jnp.where(own_col == row, o0.astype(f32), 0.0), axis=0, keepdims=True) for row in (flat[0:1], nu_row)
    )
    t0, t1 = iota2((total, 128), 0), iota2((total, 128), 1)
    lane = t1.astype(f32)
    lane1 = lane[0:1]
    before = t0 < t1

    def steps(row, size, count):
        return sum(jnp.where(row >= float(size * q), 1.0, 0.0) for q in range(1, count))

    def col(row):
        return jnp.sum(jnp.where(t0 == t1, row, 0.0), axis=1, keepdims=True)

    def down(mask, value=1.0):
        return jnp.sum(jnp.where(mask, value, 0.0), axis=0, keepdims=True)

    dead = -1.0 - lane1
    to_chip = steps(place, 2 * per_owner, chips)
    from_chip = steps(lane1, cap, chips)
    key = jnp.where(live_row, place, dead)
    pair = jnp.where(live_row, from_chip * chips + to_chip, dead)
    dest = jnp.where(live_row, to_chip, dead)
    key_col, pair_col, dest_col, from_col = col(key), col(pair), col(dest), col(from_chip)
    same = key_col == key
    pos = down((pair_col == pair) & before)
    copies = down(same & before)
    first = jnp.where(live_row & (copies == 0.0), 1.0, 0.0)
    first_col = col(first) > 0
    order = down(first_col & (dest_col == dest) & before)
    rank = down(same & first_col, col(order))
    pos_col, copies_col, rank_col = col(pos), col(copies), col(rank)
    mine = dest_col == chip
    hit = mine & (rank_col == lane)
    loc = jnp.where(hit, from_col * cap + pos_col - zero_slab, 0.0)

    def put(row, value):
        tab_ref[row:row + 1, :] = value.astype(jnp.int32)

    for j in range(most):
        put(j, down(copies_col == float(j), loc) + zero_slab)
    put(most, down(hit & first_col, col(place) - 2 * per_owner * chip))
    slot_col = t0.astype(f32)[:, 0:1] - cap * chip
    for q in range(chips):
        put(most + 1 + q, down((from_col == chip) & (dest_col == float(q)) & (pos_col == lane), slot_col))

    def top(row):
        return jnp.max(jnp.where(live_row, row, 0.0), axis=1, keepdims=True)

    crossing = jnp.where(to_chip == from_chip, 0.0, pos + 1.0)
    sizes = (top(rank + 1.0), top(copies + 1.0), top(crossing))
    which, missed = jnp.zeros((1, 1), f32), jnp.ones((1, 1), f32)
    for limits in variants[:-1]:
        over = sum(jnp.where(size > float(limit), 1.0, 0.0) for size, limit in zip(sizes, limits))
        missed = jnp.where(over > 0, missed, 0.0)
        which = which + missed
    which_ref[...] = which.astype(jnp.int32)
    return place_mu


def prep_kernel(
    n, variants, pairs_hbm, counts_hbm, owned_hbm, occ_hbm, tab_ref, lhs, which_ref,
    pairs_ref, counts_ref, owned_ref, mscr, msnd, mall, occ_all, i_sem, m_s, m_r, o_s, o_r,
):
    me = lax.axis_index("ao")
    slots = pairs_ref.shape[1]
    per_owner = owned_ref.shape[1]
    rows = occ_hbm.shape[0]
    occupied = rows // per_owner
    barrier = pltpu.get_barrier_semaphore()
    for k in range(1, n):
        pl.semaphore_signal(barrier, inc=1, device_id={"ao": lax.rem(me + k, n)}, device_id_type=MESH)
    own_occ = occ_all.at[me]
    inputs = [
        pltpu.make_async_copy(src, dst, i_sem.at[i]) for i, (src, dst) in enumerate((
            (pairs_hbm, pairs_ref), (counts_hbm, counts_ref), (owned_hbm, owned_ref), (occ_hbm, own_occ),
        ))
    ]
    for copy in inputs:
        copy.start()
    for copy in inputs:
        copy.wait()
    mscr[...] = jnp.zeros(mscr.shape, jnp.int32)
    mscr[0:2, 0:slots] = pairs_ref[...]
    mscr[2:3, 0:slots] = jnp.where(iota2((1, slots), 1) < counts_ref[...], 1, 0)
    mscr[3:4, 0:per_owner] = owned_ref[...]
    meta = mscr[...]
    by_slot, by_owner = pltpu.roll(meta, me * slots, 1), pltpu.roll(meta, me * per_owner, 1)
    meta = jnp.where(iota2(meta.shape, 0) == 3, by_owner, by_slot)
    msnd[...] = meta
    mall[me] = meta
    with jax.named_scope("barrier"):
        pl.semaphore_wait(barrier, n - 1)
    sent = []
    for k in range(1, n):
        to = {"ao": lax.rem(me + k, n)}
        for src, dst, ss, rs in ((msnd, mall, m_s, m_r), (own_occ, occ_all, o_s, o_r)):
            copy = pltpu.make_async_remote_copy(
                src_ref=src, dst_ref=dst.at[me], send_sem=ss.at[k], recv_sem=rs.at[k],
                device_id=to, device_id_type=MESH,
            )
            copy.start()
            sent.append(copy)
    with jax.named_scope("meta_wait"):
        for copy in sent:
            copy.wait_recv()
    flat = mall[0]
    for r in range(1, n):
        flat = flat + mall[r]
    chip = (me // 2).astype(f32)
    with jax.named_scope("tables"):
        place_mu = make_tables(n, slots, per_owner, chip, variants, flat, tab_ref, which_ref)

    pair_rows = 2 * occupied * slots
    r0, r1 = iota2((pair_rows, 128), 0), iota2((pair_rows, 128), 1)
    mine = r1 == me * slots + r0 // (2 * occupied)
    want = jnp.sum(jnp.where(mine, place_mu, 0.0), axis=1, keepdims=True) * occupied
    wide = (pair_rows, n * rows)
    want = want + (lax.rem(r0, occupied)).astype(f32)[:, 0:1]
    pick = jnp.where(iota2(wide, 1).astype(f32) == want, 1.0, 0.0).astype(bf16)
    occ = occ_all[...].reshape(n * rows, 128)
    picked = jnp.dot(pick, occ, preferred_element_type=f32)
    upper = lax.rem(r0 // occupied, 2) == 0
    lhs[:, 0:128] = jnp.where(upper, picked, 0.0).astype(bf16)
    lhs[:, 128:256] = jnp.where(upper, 0.0, picked).astype(bf16)

    for copy in sent:
        copy.wait_send()


def prepare(n, variants, pairs, counts, owned, occ):
    slots = pairs.shape[0]
    per_owner, occupied, width = occ.shape
    rows = per_owner * occupied
    dma, vm = pltpu.SemaphoreType.DMA, pltpu.VMEM
    whole = pl.BlockSpec(memory_space=pltpu.VMEM)
    return pl.pallas_call(
        functools.partial(prep_kernel, n, variants),
        out_shape=(
            jax.ShapeDtypeStruct((TAB_ROWS, 128), jnp.int32),
            jax.ShapeDtypeStruct((2 * occupied * slots, 2 * width), bf16),
            jax.ShapeDtypeStruct((1, 1), jnp.int32),
        ),
        in_specs=[pl.BlockSpec(memory_space=pl.ANY)] * 4,
        out_specs=(whole,) * 3,
        scratch_shapes=[
            vm((2, slots), jnp.int32), vm((1, 1), jnp.int32), vm((1, per_owner), jnp.int32),
            vm((8, 128), jnp.int32), vm((8, 128), jnp.int32), vm((n, 8, 128), jnp.int32),
            vm((n, rows, width), bf16),
            dma((4,)), dma((n,)), dma((n,)), dma((n,)), dma((n,)),
        ],
        compiler_params=pltpu.CompilerParams(
            collective_id=0, has_side_effects=True, vmem_limit_bytes=62 * 1024 * 1024,
        ),
    )(pairs.T, counts.reshape(1, 1), owned.reshape(1, per_owner), occ.reshape(rows, width))


def cuts(span):
    out, at = [], 0
    for part in CHUNKS:
        out.append((at, part * span // 8))
        at += part * span // 8
    return out


def make_plan(count):
    out = ["H0"]
    for c in range(1, count + 1):
        out += ["H%d" % c] + ["W"] * (c == count - 1) + ["P%d" % (c - 1)]
    out += ["A0", "A1", "F0", "A2", "F1", "V", "A3", "F2", "M0"]
    for c in range(count):
        out += ["A%d" % (c + 4), "F%d" % (c + 3), "M%d" % (c + 1), "X%d" % c, "Y%d" % (c - 1)]
        out += ["S%d" % (c - 2), "T%d" % (c - 3)]
    late = ["Y%d" % (count - 3), "X%d" % (count - 1)]
    out = [name for name in out if name not in late]
    at = out.index("X%d" % (count - 2)) + 1
    out[at:at] = late[::-1]
    out += ["Y%d" % (count - 1)]
    out += ["S%d" % c for c in range(count - 2, count)] + ["T%d" % c for c in range(count - 3, count)]
    return [name for name in out if len(name) == 1 or 0 <= int(name[1:]) < count]


def main_kernel(n, nz, kept, depth_j, cross, tab_ref, lhs_ref, blk_hbm, vir_hbm, out_hbm, out_ref, out_sem, *refs):
    (vir_both, vir, blk, hsnd, snd, rows, part, rx, ry, tx, ty, vir_sem, vir_s, vir_r, b_sem, h_s, h_r, a_s, a_r,
     z_s, z_r, c_s, far_r, near_r) = refs[:24]
    pieces = refs[24:]
    count = len(pieces) // 2
    slab, rcv = pieces[:count], pieces[count:]
    me, z = lax.axis_index("ao"), lax.axis_index("aux")
    core, chip = lax.rem(me, 2), me // 2
    cx, cy = lax.rem(chip, 2), chip // 2
    mate = me + 1 - 2 * core
    xmate = me + 2 - 4 * cx
    ymate = me + 4 - 8 * cy
    others = (xmate, ymate, xmate + 4 - 8 * cy)
    slots, span, width = hsnd.shape
    cap = 2 * slots
    deep = blk.shape[1] // 2
    occupied = span // deep
    group = 2 * occupied
    per_owner = vir_hbm.shape[0]
    most = n * CAP
    zero_slab = n // 2 * cap
    chunks = cuts(span)
    edge = (z < 1) | (z + 1 >= nz)
    inner = jnp.logical_not(edge)

    barrier = pltpu.get_barrier_semaphore()
    for to in (mate,) + others:
        pl.semaphore_signal(barrier, inc=1, device_id={"ao": to}, device_id_type=MESH)

    for d in (1, 2):
        @pl.when(z + d < nz)
        def _():
            pl.semaphore_signal(barrier, inc=1, device_id={"aux": z + d}, device_id_type=MESH)

        @pl.when(z - d >= 0)
        def _():
            pl.semaphore_signal(barrier, inc=1, device_id={"aux": z - d}, device_id_type=MESH)

    for c, (at, step) in enumerate(chunks):
        for half in range(2):
            these = pl.ds(half * deep + at // occupied, step // occupied)
            pltpu.make_async_copy(blk_hbm.at[:, these], blk.at[:, these], b_sem.at[c]).start()
    own_vir = vir_both.at[pl.ds(core * per_owner, per_owner)]
    vir_copy = pltpu.make_async_copy(vir_hbm, own_vir, vir_sem)
    vir_copy.start()

    def remote(src, dst, ss, rs, to):
        copy = pltpu.make_async_remote_copy(
            src_ref=src, dst_ref=dst, send_sem=ss, recv_sem=rs, device_id={"ao": to}, device_id_type=MESH,
        )
        copy.start()
        return copy

    def await_bytes(like, sem):
        pltpu.make_async_copy(like, like, sem).wait()

    h_copies, vir_pass = {}, []

    def stage_h(c):
        at, step = chunks[c]

        def product(s, half, q):
            right = blk[s, pl.ds(half * deep + at // occupied + 2 * q, 2)].reshape(2 * width, width)
            left = lhs_ref[pl.ds(pl.multiple_of(s * group, group), group), :]
            return jnp.dot(left, right, preferred_element_type=f32).astype(bf16)

        await_bytes(blk.at[:, pl.ds(0, 2 * step // occupied)], b_sem.at[c])

        @pl.loop(0, slots, unroll=3)
        def _(s):
            for q in range(step // group):
                hsnd[s, at + q * group:at + (q + 1) * group, :] = product(s, 1 - core, q)
                slab[c][core * slots + s, q * group:(q + 1) * group, :] = product(s, core, q)

        if c == 0:
            for at_edge, signals in ((edge, 6), (inner, 7)):
                @pl.when(at_edge)
                def _():
                    pl.semaphore_wait(barrier, signals)
        h_copies[c] = remote(
            hsnd.at[:, pl.ds(at, step), :], slab[c].at[pl.ds(core * slots, slots)], h_s.at[c], h_r.at[c], mate,
        )

    def stage_p(c):
        at, step = chunks[c]
        h_copies[c].wait_recv()
        for d, to in enumerate(others):
            for j in range(cross):
                snd[d, j, at:at + step, :] = slab[c][tab_ref[most + 1 + to // 2, j]]
        for d, to in enumerate(others):
            remote(snd.at[d, :, pl.ds(at, step), :], rcv[c].at[pl.ds(chip * cap, cross)], a_s.at[c], a_r.at[c], to)
        for j in range(cap):
            rcv[c][chip * cap + j] = slab[c][tab_ref[most + 1 + chip, j]]
        rcv[c][zero_slab] = jnp.zeros((step, width), bf16)

    def stage_w():
        vir_copy.wait()
        vir_pass.append(remote(own_vir, own_vir, vir_s, vir_r, mate))

    def z_copy(c, d, up):
        src = z if d < 3 else z - 2 if up else z + 2
        hop = min(d, 2) if d < 3 else 1
        passing = jnp.where(edge, 1, 0) if d == 2 else 0
        return pltpu.make_async_remote_copy(
            src_ref=rows.at[src, pl.ds(*chunks[c])], dst_ref=rows.at[src, pl.ds(*chunks[c])],
            send_sem=z_s.at[c], recv_sem=z_r.at[c, passing],
            device_id={"aux": z + hop if up else z - hop}, device_id_type=MESH,
        )

    def z_sends(d, up):
        if d < 3:
            return z + d < nz if up else z - d >= 0
        return (z >= 2) & (z + 1 < nz) if up else (z + 2 < nz) & (z >= 1)

    def z_start(c, d):
        for up in (True, False):
            @pl.when(z_sends(d, up))
            def _():
                z_copy(c, d, up).start()

    def z_bytes(c, units):
        return rows.at[pl.ds(0, units), pl.ds(*chunks[c])]

    def stage_f(c):
        @pl.when(inner)
        def _():
            await_bytes(z_bytes(c, 1), z_r.at[c, 1])

        z_start(c, 3)

    def z_rest(c):
        for at_edge, units in ((edge, 3), (inner, 2)):
            @pl.when(at_edge)
            def _():
                await_bytes(z_bytes(c, units), z_r.at[c, 0])

    def stage_a(c):
        at, step = chunks[c]
        await_bytes(snd.at[:, :, pl.ds(at, step), :], a_r.at[c])

        @pl.loop(0, kept)
        def _(k):
            acc = rcv[c][tab_ref[0, k]].astype(f32)
            for j in range(1, depth_j):
                acc = acc + rcv[c][tab_ref[j, k]].astype(f32)
            rows[z, at:at + step, pl.ds(pl.multiple_of(k * width, width), width)] = acc.astype(bf16)

        z_start(c, 2)
        z_start(c, 1)

    o_copies = {}
    tile = 256
    depth = rows.shape[-1]
    piece = 16

    def stage_v():
        vir_pass[0].wait_recv()

        @pl.loop(0, width // piece)
        def _(i):
            at = pl.ds(pl.multiple_of(i * piece, piece), piece)
            for k in range(kept):
                to = pl.ds(pl.multiple_of(k * width + i * piece, piece), piece)
                vir[to, :] = vir_both[tab_ref[most, k], at, :]

    def stage_m(c):
        at, step = chunks[c]
        mid = step // 2
        lo, hi, here = pl.ds(at, mid), pl.ds(at + mid, mid), pl.ds(at // 2, mid)

        with jax.named_scope("Z"):
            z_rest(c)

        far = 2 * (1 - cy) + 1 - cx
        sends = (
            (far, lo, rx.at[0, here], far_r, xmate), (far, hi, ry.at[0, here], far_r, ymate),
            (2 * cy + 1 - cx, lo, rx.at[1, here], near_r, xmate),
            (2 * (1 - cy) + cx, hi, ry.at[1, here], near_r, ymate),
        )
        tiles = vir.shape[1] // tile
        half = tiles // 2

        def send(first, last):
            cols = pl.ds(first * tile, (last - first) * tile)
            for which, these, dst, sem, to in sends:
                remote(part.at[which, these, cols], dst.at[:, cols], c_s.at[c], sem.at[c], to)

        @pl.loop(0, tiles)
        def _(j):
            cols = pl.ds(pl.multiple_of(j * tile, tile), tile)
            left = rows[:, at:at + step, :].reshape(nz * step, depth)
            got = jnp.dot(left, vir[:, cols], preferred_element_type=f32)
            part[:, at:at + step, cols] = got.astype(bf16).reshape(nz, step, tile)

            @pl.when(j == half - 1)
            def _():
                send(0, half)

        send(half, tiles)

    def add2(a, b):
        return (a.astype(f32) + b.astype(f32)).astype(bf16)

    def stage_x(c):
        at, step = chunks[c]
        mid = step // 2
        here, there = slice(at // 2, at // 2 + mid), pl.ds(at // 2, mid)
        await_bytes(part.at[0, pl.ds(at, step)], far_r.at[c])
        tx[here] = add2(part[2 * (1 - cy) + cx, at:at + mid], rx[0, here])
        ty[here] = add2(part[2 * cy + 1 - cx, at + mid:at + step], ry[0, here])
        remote(tx.at[there], rx.at[2, there], c_s.at[c], near_r.at[c], ymate)
        remote(ty.at[there], ry.at[2, there], c_s.at[c], near_r.at[c], xmate)

    def stage_y(c):
        at, step = chunks[c]
        mid = step // 2
        here = slice(at // 2, at // 2 + mid)
        await_bytes(part.at[pl.ds(0, 2), pl.ds(at, step)], near_r.at[c])
        top = part[chip, at:at + mid].astype(f32) + rx[1, here].astype(f32) + rx[2, here].astype(f32)
        low = part[chip, at + mid:at + step].astype(f32) + ry[1, here].astype(f32) + ry[2, here].astype(f32)
        out_ref[at:at + mid, :] = top.astype(bf16)
        out_ref[at + mid:at + step, :] = low.astype(bf16)
        o_copies[c] = pltpu.make_async_copy(out_ref.at[pl.ds(at, step)], out_hbm.at[pl.ds(at, step)], out_sem.at[c])
        o_copies[c].start()

    def stage_s(c):
        h_copies[c].wait_send()
        await_bytes(snd.at[:, :, pl.ds(*chunks[c]), :], a_s.at[c])
        for at_edge, units in ((edge, 2), (inner, 4)):
            @pl.when(at_edge)
            def _():
                await_bytes(z_bytes(c, units), z_s.at[c])

    def stage_t(c):
        await_bytes(part.at[pl.ds(0, 3), pl.ds(*chunks[c])], c_s.at[c])
        o_copies[c].wait()

    run = {"H": stage_h, "P": stage_p, "W": stage_w, "A": stage_a, "F": stage_f, "M": stage_m, "X": stage_x,
           "Y": stage_y, "V": stage_v, "S": stage_s, "T": stage_t}
    for item in make_plan(count):
        with jax.named_scope(item):
            run[item[0]](*[int(v) for v in item[1:]])
    vir_pass[0].wait_send()


def fused(n, nz, sizes, call_id, tab, lhs, blocks, vir3):
    kept, depth_j, cross = sizes
    slots, deep, _, width = blocks.shape
    per_owner, _, columns = vir3.shape
    span = deep * lhs.shape[0] // slots // 4
    steps = [step for _, step in cuts(span)]
    count, cap = len(steps), 2 * slots
    dma, vm = pltpu.SemaphoreType.DMA, pltpu.VMEM
    anywhere, whole = pl.BlockSpec(memory_space=pl.ANY), pl.BlockSpec(memory_space=pltpu.VMEM)
    return pl.pallas_call(
        functools.partial(main_kernel, n, nz, kept, depth_j, cross),
        out_shape=jax.ShapeDtypeStruct((span, columns), bf16),
        in_specs=[pl.BlockSpec(memory_space=pltpu.SMEM), whole, anywhere, anywhere],
        out_specs=anywhere,
        scratch_shapes=[
            vm((span, columns), bf16), dma((count,)),
            vm((2 * per_owner, width, columns), bf16),
            vm((kept * width, columns), bf16),
            vm(blocks.shape, bf16),
            vm((slots, span, width), bf16),
            vm((3, cross, span, width), bf16),
            vm((nz, span, kept * width), bf16),
            vm((nz, span, columns), bf16),
            vm((3, span // 2, columns), bf16),
            vm((3, span // 2, columns), bf16),
            vm((span // 2, columns), bf16),
            vm((span // 2, columns), bf16),
            dma, dma, dma,
            dma((count,)), dma((count,)), dma((count,)), dma((count,)), dma((count,)),
            dma((count,)), dma((count, 2)), dma((count,)), dma((count,)), dma((count,)),
        ] + [vm((cap, step, width), bf16) for step in steps] + [
            vm((n // 2 * cap + 1, step, width), bf16) for step in steps
        ],
        compiler_params=pltpu.CompilerParams(
            collective_id=call_id, has_side_effects=True, vmem_limit_bytes=62 * 1024 * 1024,
        ),
    )(tab, lhs, blocks, vir3)


def per_device(blocks, pairs, counts, owned_blocks, occ_coef, vir_coef):
    groups, nz = lax.axis_size("ao"), lax.axis_size("aux")
    slots, _, _, width = blocks.shape
    per_owner, occupied, _ = occ_coef.shape
    variants = VARIANTS + ((2 * per_owner, groups * CAP, 2 * slots),)
    tab, lhs, which = prepare(groups, variants, pairs, counts, owned_blocks, occ_coef)
    vir3 = vir_coef.reshape(per_owner, width, vir_coef.shape[1])
    out = lax.switch(
        which.reshape(()), [functools.partial(fused, groups, nz, v, 1 + i) for i, v in enumerate(variants)],
        tab, lhs, blocks, vir3,
    )
    return out.reshape(-1, occupied, vir_coef.shape[1])


def per_device_general(blocks, pairs, counts, owned_blocks, occ_coef, vir_coef):
    groups = lax.axis_size("ao")
    own_index = lax.axis_index("ao")
    slot_count = blocks.shape[0]
    aux_depth = blocks.shape[1]
    block_width = blocks.shape[3]
    occupied = occ_coef.shape[1]
    all_pairs, all_counts, all_owned = (
        lax.all_gather(pairs, "ao", axis=0, tiled=True),
        lax.all_gather(counts, "ao", axis=0, tiled=True),
        lax.all_gather(owned_blocks, "ao", axis=0, tiled=True),
    )
    occ_all = lax.all_gather(occ_coef, "ao", axis=0, tiled=True)
    per_owner = all_owned.shape[0] // groups
    slot_ids = jnp.arange(slot_count, dtype=jnp.int32)
    in_use = slot_ids < counts[0]
    occ_pick = occ_all[block_place(pairs[:, 0], all_owned)]
    slab_values = jnp.einsum("sim,spmn->spin", occ_pick, blocks, preferred_element_type=jnp.float32)
    slab_values = jnp.where(in_use[:, None, None, None], slab_values, 0.0).astype(jnp.bfloat16)
    flat_slabs = slab_values.reshape(slot_count, aux_depth * occupied, block_width)
    place_all = block_place(all_pairs[:, 1], all_owned).reshape(groups, slot_count)
    owner_all = place_all // per_owner
    local_all = place_all % per_owner
    live_all = slot_ids[None, :] < all_counts[:, None]
    mine_all = live_all & (owner_all == own_index)
    local_ids = jnp.arange(per_owner, dtype=jnp.int32)
    slabs_got = lax.all_gather(flat_slabs, "ao", axis=0, tiled=True)
    assign = (
        mine_all.reshape(-1)[None, :] & (local_all.reshape(-1)[None, :] == local_ids[:, None])
    ).astype(jnp.bfloat16)
    summed = jnp.einsum("lt,tqm->qlm", assign, slabs_got, preferred_element_type=jnp.float32)
    rows_local = summed.reshape(summed.shape[0], per_owner * block_width).astype(jnp.bfloat16)
    rows_whole = lax.all_gather(rows_local, "aux", axis=0, tiled=True)
    share = rows_whole.shape[0] // groups
    result = lax.psum_scatter(
        jnp.dot(rows_whole, vir_coef, preferred_element_type=jnp.float32).astype(jnp.bfloat16),
        "ao",
        scatter_dimension=0,
        tiled=True,
    )
    return result.reshape(share // occupied, occupied, vir_coef.shape[1])


def solution(mesh):
    in_specs = (
        P("ao", "aux", None, None),
        P("ao", None),
        P("ao"),
        P("ao"),
        P("ao", None, None),
        P("ao", "aux"),
    )
    out_specs = P("ao", None, "aux")
    small = mesh.shape["ao"] == 8 and mesh.shape["aux"] == 4
    body = per_device if small else per_device_general
    return jax.shard_map(body, mesh=mesh, in_specs=in_specs, out_specs=out_specs, check_vma=False)
```

```python
import functools

import jax
import jax.numpy as jnp
from jax import lax
from jax.experimental import pallas as pl
from jax.experimental.pallas import tpu as pltpu
from jax.sharding import PartitionSpec as P

MESH = pl.DeviceIdType.MESH
CAP = 3
CHUNKS = (1,) * 8
VARIANTS = ((8, 4, 6), (9, 4, 6), (10, 4, 6), (12, 6, 6), (12, 6, 9))
TAB_ROWS = 32
f32 = jnp.float32
bf16 = jnp.bfloat16


def block_place(block_ids, owned_all):
    hits = block_ids[..., None] == owned_all
    positions = jnp.arange(owned_all.shape[0], dtype=jnp.int32)
    return jnp.sum(jnp.where(hits, positions, 0), axis=-1)


def iota2(shape, axis):
    return lax.broadcasted_iota(jnp.int32, shape, axis)


def make_tables(n, slots, per_owner, chip, variants, flat, tab_ref, which_ref):
    total, owned, cap = n * slots, n * per_owner, 2 * slots
    chips, most, zero_slab = n // 2, n * CAP, n * slots
    flat = flat.astype(f32)
    nu_row, live_row, own_row = flat[1:2], flat[2:3] > 0, flat[3:4]
    o0, o1 = iota2((owned, 128), 0), iota2((owned, 128), 1)
    own_col = jnp.sum(jnp.where(o0 == o1, own_row, 0.0), axis=1, keepdims=True)
    place_mu, place = (
        jnp.sum(jnp.where(own_col == row, o0.astype(f32), 0.0), axis=0, keepdims=True) for row in (flat[0:1], nu_row)
    )
    t0, t1 = iota2((total, 128), 0), iota2((total, 128), 1)
    lane = t1.astype(f32)
    lane1 = lane[0:1]
    before = t0 < t1

    def steps(row, size, count):
        return sum(jnp.where(row >= float(size * q), 1.0, 0.0) for q in range(1, count))

    def col(row):
        return jnp.sum(jnp.where(t0 == t1, row, 0.0), axis=1, keepdims=True)

    def down(mask, value=1.0):
        return jnp.sum(jnp.where(mask, value, 0.0), axis=0, keepdims=True)

    dead = -1.0 - lane1
    to_chip = steps(place, 2 * per_owner, chips)
    from_chip = steps(lane1, cap, chips)
    key = jnp.where(live_row, place, dead)
    pair = jnp.where(live_row, from_chip * chips + to_chip, dead)
    dest = jnp.where(live_row, to_chip, dead)
    key_col, pair_col, dest_col, from_col = col(key), col(pair), col(dest), col(from_chip)
    same = key_col == key
    pos = down((pair_col == pair) & before)
    copies = down(same & before)
    first = jnp.where(live_row & (copies == 0.0), 1.0, 0.0)
    first_col = col(first) > 0
    order = down(first_col & (dest_col == dest) & before)
    rank = down(same & first_col, col(order))
    pos_col, copies_col, rank_col = col(pos), col(copies), col(rank)
    mine = dest_col == chip
    hit = mine & (rank_col == lane)
    loc = jnp.where(hit, from_col * cap + pos_col - zero_slab, 0.0)

    def put(row, value):
        tab_ref[row:row + 1, :] = value.astype(jnp.int32)

    for j in range(most):
        put(j, down(copies_col == float(j), loc) + zero_slab)
    put(most, down(hit & first_col, col(place) - 2 * per_owner * chip))
    slot_col = t0.astype(f32)[:, 0:1] - cap * chip
    for q in range(chips):
        put(most + 1 + q, down((from_col == chip) & (dest_col == float(q)) & (pos_col == lane), slot_col))

    def top(row):
        return jnp.max(jnp.where(live_row, row, 0.0), axis=1, keepdims=True)

    crossing = jnp.where(to_chip == from_chip, 0.0, pos + 1.0)
    sizes = (top(rank + 1.0), top(copies + 1.0), top(crossing))
    which, missed = jnp.zeros((1, 1), f32), jnp.ones((1, 1), f32)
    for limits in variants[:-1]:
        over = sum(jnp.where(size > float(limit), 1.0, 0.0) for size, limit in zip(sizes, limits))
        missed = jnp.where(over > 0, missed, 0.0)
        which = which + missed
    which_ref[...] = which.astype(jnp.int32)
    return place_mu


def prep_kernel(
    n, variants, pairs_hbm, counts_hbm, owned_hbm, occ_hbm, tab_ref, lhs, which_ref,
    pairs_ref, counts_ref, owned_ref, mscr, msnd, mall, occ_all, i_sem, m_s, m_r, o_s, o_r,
):
    me = lax.axis_index("ao")
    slots = pairs_ref.shape[1]
    per_owner = owned_ref.shape[1]
    rows = occ_hbm.shape[0]
    occupied = rows // per_owner
    barrier = pltpu.get_barrier_semaphore()
    for k in range(1, n):
        pl.semaphore_signal(barrier, inc=1, device_id={"ao": lax.rem(me + k, n)}, device_id_type=MESH)
    own_occ = occ_all.at[me]
    inputs = [
        pltpu.make_async_copy(src, dst, i_sem.at[i]) for i, (src, dst) in enumerate((
            (pairs_hbm, pairs_ref), (counts_hbm, counts_ref), (owned_hbm, owned_ref), (occ_hbm, own_occ),
        ))
    ]
    for copy in inputs:
        copy.start()
    for copy in inputs:
        copy.wait()
    mscr[...] = jnp.zeros(mscr.shape, jnp.int32)
    mscr[0:2, 0:slots] = pairs_ref[...]
    mscr[2:3, 0:slots] = jnp.where(iota2((1, slots), 1) < counts_ref[...], 1, 0)
    mscr[3:4, 0:per_owner] = owned_ref[...]
    meta = mscr[...]
    by_slot, by_owner = pltpu.roll(meta, me * slots, 1), pltpu.roll(meta, me * per_owner, 1)
    meta = jnp.where(iota2(meta.shape, 0) == 3, by_owner, by_slot)
    msnd[...] = meta
    mall[me] = meta
    with jax.named_scope("barrier"):
        pl.semaphore_wait(barrier, n - 1)
    for k in range(1, n):
        to = {"ao": lax.rem(me + k, n)}
        for src, dst, ss, rs in ((msnd, mall, m_s, m_r), (own_occ, occ_all, o_s, o_r)):
            copy = pltpu.make_async_remote_copy(
                src_ref=src, dst_ref=dst.at[me], send_sem=ss, recv_sem=rs,
                device_id=to, device_id_type=MESH,
            )
            copy.start()

    def await_others(sems):
        for like, sem in zip((mall, occ_all), sems):
            like = like.at[pl.ds(0, n - 1)]
            pltpu.make_async_copy(like, like, sem).wait()

    with jax.named_scope("meta_wait"):
        await_others((m_r, o_r))
    flat = mall[0]
    for r in range(1, n):
        flat = flat + mall[r]
    chip = (me // 2).astype(f32)
    with jax.named_scope("tables"):
        place_mu = make_tables(n, slots, per_owner, chip, variants, flat, tab_ref, which_ref)

    pair_rows = 2 * occupied * slots
    r0, r1 = iota2((pair_rows, 128), 0), iota2((pair_rows, 128), 1)
    mine = r1 == me * slots + r0 // (2 * occupied)
    want = jnp.sum(jnp.where(mine, place_mu, 0.0), axis=1, keepdims=True) * occupied
    wide = (pair_rows, n * rows)
    want = want + (lax.rem(r0, occupied)).astype(f32)[:, 0:1]
    pick = jnp.where(iota2(wide, 1).astype(f32) == want, 1.0, 0.0).astype(bf16)
    occ = occ_all[...].reshape(n * rows, 128)
    picked = jnp.dot(pick, occ, preferred_element_type=f32)
    upper = lax.rem(r0 // occupied, 2) == 0
    lhs[:, 0:128] = jnp.where(upper, picked, 0.0).astype(bf16)
    lhs[:, 128:256] = jnp.where(upper, 0.0, picked).astype(bf16)

    await_others((m_s, o_s))


def prepare(n, variants, pairs, counts, owned, occ):
    slots = pairs.shape[0]
    per_owner, occupied, width = occ.shape
    rows = per_owner * occupied
    dma, vm = pltpu.SemaphoreType.DMA, pltpu.VMEM
    whole = pl.BlockSpec(memory_space=pltpu.VMEM)
    return pl.pallas_call(
        functools.partial(prep_kernel, n, variants),
        out_shape=(
            jax.ShapeDtypeStruct((TAB_ROWS, 128), jnp.int32),
            jax.ShapeDtypeStruct((2 * occupied * slots, 2 * width), bf16),
            jax.ShapeDtypeStruct((1, 1), jnp.int32),
        ),
        in_specs=[pl.BlockSpec(memory_space=pl.ANY)] * 4,
        out_specs=(whole,) * 3,
        scratch_shapes=[
            vm((2, slots), jnp.int32), vm((1, 1), jnp.int32), vm((1, per_owner), jnp.int32),
            vm((8, 128), jnp.int32), vm((8, 128), jnp.int32), vm((n, 8, 128), jnp.int32),
            vm((n, rows, width), bf16),
            dma((4,)), dma, dma, dma, dma,
        ],
        compiler_params=pltpu.CompilerParams(
            collective_id=0, has_side_effects=True, vmem_limit_bytes=62 * 1024 * 1024,
        ),
    )(pairs.T, counts.reshape(1, 1), owned.reshape(1, per_owner), occ.reshape(rows, width))


def cuts(span):
    out, at = [], 0
    for part in CHUNKS:
        out.append((at, part * span // 8))
        at += part * span // 8
    return out


def make_plan(count):
    out = ["H0"]
    for c in range(1, count + 1):
        out += ["H%d" % c] + ["W"] * (c == count - 1) + ["P%d" % (c - 1)]
    out += ["A0", "A1", "F0", "A2", "F1", "V", "A3", "F2", "M0"]
    for c in range(count):
        out += ["A%d" % (c + 4), "F%d" % (c + 3), "M%d" % (c + 1), "X%d" % c, "Y%d" % (c - 1)]
    late = ["Y%d" % (count - 3), "X%d" % (count - 1)]
    out = [name for name in out if name not in late]
    at = out.index("X%d" % (count - 2)) + 1
    out[at:at] = late[::-1]
    out += ["Y%d" % (count - 1)]
    return [name for name in out if len(name) == 1 or 0 <= int(name[1:]) < count]


def main_kernel(n, nz, kept, depth_j, cross, tab_ref, lhs_ref, blk_hbm, vir_hbm, out_hbm, out_ref, out_sem, *refs):
    (vir_both, vir, blk, hsnd, snd, rows, part, rx, ry, tx, ty, vir_sem, vir_s, vir_r, b_sem, h_s, h_r, a_s, a_r,
     z_s, z_r, c_s, far_r, near_r) = refs[:24]
    pieces = refs[24:]
    count = len(pieces) // 2
    slab, rcv = pieces[:count], pieces[count:]
    me, z = lax.axis_index("ao"), lax.axis_index("aux")
    core, chip = lax.rem(me, 2), me // 2
    cx, cy = lax.rem(chip, 2), chip // 2
    mate = me + 1 - 2 * core
    xmate = me + 2 - 4 * cx
    ymate = me + 4 - 8 * cy
    others = (xmate + 4 - 8 * cy, xmate, ymate)
    slots, span, width = hsnd.shape
    cap = 2 * slots
    deep = blk.shape[1] // 2
    occupied = span // deep
    group = 2 * occupied
    per_owner = vir_hbm.shape[0]
    most = n * CAP
    zero_slab = n // 2 * cap
    chunks = cuts(span)
    edge = (z < 1) | (z + 1 >= nz)
    inner = jnp.logical_not(edge)

    barrier = pltpu.get_barrier_semaphore()
    for to in (mate,) + others:
        pl.semaphore_signal(barrier, inc=1, device_id={"ao": to}, device_id_type=MESH)

    for d in (1, 2):
        @pl.when(z + d < nz)
        def _():
            pl.semaphore_signal(barrier, inc=1, device_id={"aux": z + d}, device_id_type=MESH)

        @pl.when(z - d >= 0)
        def _():
            pl.semaphore_signal(barrier, inc=1, device_id={"aux": z - d}, device_id_type=MESH)

    for c, (at, step) in enumerate(chunks):
        for half in range(2):
            these = pl.ds(half * deep + at // occupied, step // occupied)
            pltpu.make_async_copy(blk_hbm.at[:, these], blk.at[:, these], b_sem.at[c]).start()
    own_vir = vir_both.at[pl.ds(core * per_owner, per_owner)]
    vir_copy = pltpu.make_async_copy(vir_hbm, own_vir, vir_sem)
    vir_copy.start()

    def remote(src, dst, ss, rs, to):
        copy = pltpu.make_async_remote_copy(
            src_ref=src, dst_ref=dst, send_sem=ss, recv_sem=rs, device_id={"ao": to}, device_id_type=MESH,
        )
        copy.start()
        return copy

    def await_bytes(like, sem):
        pltpu.make_async_copy(like, like, sem).wait()

    h_copies, vir_pass = {}, []

    def stage_h(c):
        at, step = chunks[c]

        def product(s, half, q):
            right = blk[s, pl.ds(half * deep + at // occupied + 2 * q, 2)].reshape(2 * width, width)
            left = lhs_ref[pl.ds(pl.multiple_of(s * group, group), group), :]
            return jnp.dot(left, right, preferred_element_type=f32).astype(bf16)

        await_bytes(blk.at[:, pl.ds(0, 2 * step // occupied)], b_sem.at[c])

        @pl.loop(0, slots, unroll=3)
        def _(s):
            for q in range(step // group):
                hsnd[s, at + q * group:at + (q + 1) * group, :] = product(s, 1 - core, q)
                slab[c][core * slots + s, q * group:(q + 1) * group, :] = product(s, core, q)

        if c == 0:
            for at_edge, signals in ((edge, 6), (inner, 7)):
                @pl.when(at_edge)
                def _():
                    pl.semaphore_wait(barrier, signals)
        h_copies[c] = remote(
            hsnd.at[:, pl.ds(at, step), :], slab[c].at[pl.ds(core * slots, slots)], h_s, h_r.at[c], mate,
        )

    def stage_p(c):
        at, step = chunks[c]
        h_copies[c].wait_recv()
        for d, to in enumerate(others):
            for j in range(cross):
                snd[d, j, at:at + step, :] = slab[c][tab_ref[most + 1 + to // 2, j]]
        for d, to in enumerate(others):
            remote(snd.at[d, :, pl.ds(at, step), :], rcv[c].at[pl.ds(chip * cap, cross)], a_s, a_r.at[c], to)
        for j in range(cap):
            rcv[c][chip * cap + j] = slab[c][tab_ref[most + 1 + chip, j]]
        rcv[c][zero_slab] = jnp.zeros((step, width), bf16)

    def stage_w():
        vir_copy.wait()
        vir_pass.append(remote(own_vir, own_vir, vir_s, vir_r, mate))

    def z_copy(c, d, up):
        src = z if d < 3 else z - 2 if up else z + 2
        hop = min(d, 2) if d < 3 else 1
        passing = jnp.where(edge, 1, 0) if d == 2 else 0
        return pltpu.make_async_remote_copy(
            src_ref=rows.at[src, pl.ds(*chunks[c])], dst_ref=rows.at[src, pl.ds(*chunks[c])],
            send_sem=z_s, recv_sem=z_r.at[c, passing],
            device_id={"aux": z + hop if up else z - hop}, device_id_type=MESH,
        )

    def z_sends(d, up):
        if d < 3:
            return z + d < nz if up else z - d >= 0
        return (z >= 2) & (z + 1 < nz) if up else (z + 2 < nz) & (z >= 1)

    def z_start(c, d):
        for up in (True, False):
            @pl.when(z_sends(d, up))
            def _():
                z_copy(c, d, up).start()

    def z_bytes(c, units):
        return rows.at[pl.ds(0, units), pl.ds(*chunks[c])]

    def stage_f(c):
        @pl.when(inner)
        def _():
            await_bytes(z_bytes(c, 1), z_r.at[c, 1])

        z_start(c, 3)

    def z_rest(c):
        for at_edge, units in ((edge, 3), (inner, 2)):
            @pl.when(at_edge)
            def _():
                await_bytes(z_bytes(c, units), z_r.at[c, 0])

    def stage_a(c):
        at, step = chunks[c]
        await_bytes(snd.at[:, :, pl.ds(at, step), :], a_r.at[c])

        @pl.loop(0, kept)
        def _(k):
            acc = rcv[c][tab_ref[0, k]].astype(f32)
            for j in range(1, depth_j):
                acc = acc + rcv[c][tab_ref[j, k]].astype(f32)
            rows[z, at:at + step, pl.ds(pl.multiple_of(k * width, width), width)] = acc.astype(bf16)

        z_start(c, 2)
        z_start(c, 1)

    tile = 256
    depth = rows.shape[-1]
    piece = 16

    def stage_v():
        vir_pass[0].wait_recv()

        @pl.loop(0, width // piece)
        def _(i):
            at = pl.ds(pl.multiple_of(i * piece, piece), piece)
            for k in range(kept):
                to = pl.ds(pl.multiple_of(k * width + i * piece, piece), piece)
                vir[to, :] = vir_both[tab_ref[most, k], at, :]

    def stage_m(c):
        at, step = chunks[c]
        mid = step // 2
        lo, hi, here = pl.ds(at, mid), pl.ds(at + mid, mid), pl.ds(at // 2, mid)

        with jax.named_scope("Z"):
            z_rest(c)

        far = 2 * (1 - cy) + 1 - cx
        sends = (
            (far, lo, rx.at[0, here], far_r, xmate), (far, hi, ry.at[0, here], far_r, ymate),
            (2 * cy + 1 - cx, lo, rx.at[1, here], near_r, xmate),
            (2 * (1 - cy) + cx, hi, ry.at[1, here], near_r, ymate),
        )
        tiles = vir.shape[1] // tile
        half = tiles // 2

        def send(first, last):
            cols = pl.ds(first * tile, (last - first) * tile)
            for which, these, dst, sem, to in sends:
                remote(part.at[which, these, cols], dst.at[:, cols], c_s, sem.at[c], to)

        @pl.loop(0, tiles)
        def _(j):
            cols = pl.ds(pl.multiple_of(j * tile, tile), tile)
            left = rows[:, at:at + step, :].reshape(nz * step, depth)
            got = jnp.dot(left, vir[:, cols], preferred_element_type=f32)
            part[:, at:at + step, cols] = got.astype(bf16).reshape(nz, step, tile)

            @pl.when(j == half - 1)
            def _():
                send(0, half)

        send(half, tiles)

    def add2(a, b):
        return (a.astype(f32) + b.astype(f32)).astype(bf16)

    def stage_x(c):
        at, step = chunks[c]
        mid = step // 2
        here, there = slice(at // 2, at // 2 + mid), pl.ds(at // 2, mid)
        await_bytes(part.at[0, pl.ds(at, step)], far_r.at[c])
        tx[here] = add2(part[2 * (1 - cy) + cx, at:at + mid], rx[0, here])
        ty[here] = add2(part[2 * cy + 1 - cx, at + mid:at + step], ry[0, here])
        remote(tx.at[there], rx.at[2, there], c_s, near_r.at[c], ymate)
        remote(ty.at[there], ry.at[2, there], c_s, near_r.at[c], xmate)

    def stage_y(c):
        at, step = chunks[c]
        mid = step // 2
        here = slice(at // 2, at // 2 + mid)
        await_bytes(part.at[pl.ds(0, 2), pl.ds(at, step)], near_r.at[c])
        top = part[chip, at:at + mid].astype(f32) + rx[1, here].astype(f32) + rx[2, here].astype(f32)
        low = part[chip, at + mid:at + step].astype(f32) + ry[1, here].astype(f32) + ry[2, here].astype(f32)
        out_ref[at:at + mid, :] = top.astype(bf16)
        out_ref[at + mid:at + step, :] = low.astype(bf16)
        pltpu.make_async_copy(out_ref.at[pl.ds(at, step)], out_hbm.at[pl.ds(at, step)], out_sem).start()

    run = {"H": stage_h, "P": stage_p, "W": stage_w, "A": stage_a, "F": stage_f, "M": stage_m, "X": stage_x,
           "Y": stage_y, "V": stage_v}
    for item in make_plan(count):
        with jax.named_scope(item):
            run[item[0]](*[int(v) for v in item[1:]])
    vir_pass[0].wait_send()
    await_bytes(hsnd, h_s)
    await_bytes(snd, a_s)
    for at_edge, units in ((edge, 2), (inner, 4)):
        @pl.when(at_edge)
        def _():
            await_bytes(rows.at[pl.ds(0, units)], z_s)
    await_bytes(part.at[pl.ds(0, 3)], c_s)
    pltpu.make_async_copy(out_ref, out_hbm, out_sem).wait()


def fused(n, nz, sizes, call_id, tab, lhs, blocks, vir3):
    kept, depth_j, cross = sizes
    slots, deep, _, width = blocks.shape
    per_owner, _, columns = vir3.shape
    span = deep * lhs.shape[0] // slots // 4
    steps = [step for _, step in cuts(span)]
    count, cap = len(steps), 2 * slots
    dma, vm = pltpu.SemaphoreType.DMA, pltpu.VMEM
    anywhere, whole = pl.BlockSpec(memory_space=pl.ANY), pl.BlockSpec(memory_space=pltpu.VMEM)
    return pl.pallas_call(
        functools.partial(main_kernel, n, nz, kept, depth_j, cross),
        out_shape=jax.ShapeDtypeStruct((span, columns), bf16),
        in_specs=[pl.BlockSpec(memory_space=pltpu.SMEM), whole, anywhere, anywhere],
        out_specs=anywhere,
        scratch_shapes=[
            vm((span, columns), bf16), dma,
            vm((2 * per_owner, width, columns), bf16),
            vm((kept * width, columns), bf16),
            vm(blocks.shape, bf16),
            vm((slots, span, width), bf16),
            vm((3, cross, span, width), bf16),
            vm((nz, span, kept * width), bf16),
            vm((nz, span, columns), bf16),
            vm((3, span // 2, columns), bf16),
            vm((3, span // 2, columns), bf16),
            vm((span // 2, columns), bf16),
            vm((span // 2, columns), bf16),
            dma, dma, dma,
            dma((count,)), dma, dma((count,)), dma, dma((count,)),
            dma, dma((count, 2)), dma, dma((count,)), dma((count,)),
        ] + [vm((cap, step, width), bf16) for step in steps] + [
            vm((n // 2 * cap + 1, step, width), bf16) for step in steps
        ],
        compiler_params=pltpu.CompilerParams(
            collective_id=call_id, has_side_effects=True, vmem_limit_bytes=62 * 1024 * 1024,
        ),
    )(tab, lhs, blocks, vir3)


def per_device(blocks, pairs, counts, owned_blocks, occ_coef, vir_coef):
    groups, nz = lax.axis_size("ao"), lax.axis_size("aux")
    slots, _, _, width = blocks.shape
    per_owner, occupied, _ = occ_coef.shape
    variants = VARIANTS + ((2 * per_owner, groups * CAP, 2 * slots),)
    tab, lhs, which = prepare(groups, variants, pairs, counts, owned_blocks, occ_coef)
    vir3 = vir_coef.reshape(per_owner, width, vir_coef.shape[1])
    out = lax.switch(
        which.reshape(()), [functools.partial(fused, groups, nz, v, 1 + i) for i, v in enumerate(variants)],
        tab, lhs, blocks, vir3,
    )
    return out.reshape(-1, occupied, vir_coef.shape[1])


def per_device_general(blocks, pairs, counts, owned_blocks, occ_coef, vir_coef):
    groups = lax.axis_size("ao")
    own_index = lax.axis_index("ao")
    slot_count = blocks.shape[0]
    aux_depth = blocks.shape[1]
    block_width = blocks.shape[3]
    occupied = occ_coef.shape[1]
    all_pairs, all_counts, all_owned = (
        lax.all_gather(pairs, "ao", axis=0, tiled=True),
        lax.all_gather(counts, "ao", axis=0, tiled=True),
        lax.all_gather(owned_blocks, "ao", axis=0, tiled=True),
    )
    occ_all = lax.all_gather(occ_coef, "ao", axis=0, tiled=True)
    per_owner = all_owned.shape[0] // groups
    slot_ids = jnp.arange(slot_count, dtype=jnp.int32)
    in_use = slot_ids < counts[0]
    occ_pick = occ_all[block_place(pairs[:, 0], all_owned)]
    slab_values = jnp.einsum("sim,spmn->spin", occ_pick, blocks, preferred_element_type=jnp.float32)
    slab_values = jnp.where(in_use[:, None, None, None], slab_values, 0.0).astype(jnp.bfloat16)
    flat_slabs = slab_values.reshape(slot_count, aux_depth * occupied, block_width)
    place_all = block_place(all_pairs[:, 1], all_owned).reshape(groups, slot_count)
    owner_all = place_all // per_owner
    local_all = place_all % per_owner
    live_all = slot_ids[None, :] < all_counts[:, None]
    mine_all = live_all & (owner_all == own_index)
    local_ids = jnp.arange(per_owner, dtype=jnp.int32)
    slabs_got = lax.all_gather(flat_slabs, "ao", axis=0, tiled=True)
    assign = (
        mine_all.reshape(-1)[None, :] & (local_all.reshape(-1)[None, :] == local_ids[:, None])
    ).astype(jnp.bfloat16)
    summed = jnp.einsum("lt,tqm->qlm", assign, slabs_got, preferred_element_type=jnp.float32)
    rows_local = summed.reshape(summed.shape[0], per_owner * block_width).astype(jnp.bfloat16)
    rows_whole = lax.all_gather(rows_local, "aux", axis=0, tiled=True)
    share = rows_whole.shape[0] // groups
    result = lax.psum_scatter(
        jnp.dot(rows_whole, vir_coef, preferred_element_type=jnp.float32).astype(jnp.bfloat16),
        "ao",
        scatter_dimension=0,
        tiled=True,
    )
    return result.reshape(share // occupied, occupied, vir_coef.shape[1])


def solution(mesh):
    in_specs = (
        P("ao", "aux", None, None),
        P("ao", None),
        P("ao"),
        P("ao"),
        P("ao", None, None),
        P("ao", "aux"),
    )
    out_specs = P("ao", None, "aux")
    small = mesh.shape["ao"] == 8 and mesh.shape["aux"] == 4
    body = per_device if small else per_device_general
    return jax.shard_map(body, mesh=mesh, in_specs=in_specs, out_specs=out_specs, check_vma=False)
```
